128 devices in a mesh: col: 16 (over z, x), row: 8 (over y, core).
Axes of the slice: x: 4, y: 4, z: 4, core: 2. Of those that a mesh axis runs over, the one named last changes fastest.
Arguments:
- parent_front: float32 [12288, 12288], P('row', 'col'), as said below
- child_blocks: float32 [8192, 16384], P('row', 'col'), as said below
- child_map: int32 [2, 64], replicated, may hold values from 0 to 95, as said below
- child_order: int32 [2], replicated, may hold values from 4096 to 8192, as said below
Outputs:
- factored: float32 [12288, 12288], P('row', 'col')
The draws below stay inside these ranges and needn't reach their ends.
Inputs may be any that keep to these rules, and one draw needn't show every extreme that they name: parent_front is symmetric. `child_blocks`: each child's block, in true tile order, is symmetric. `child_map`: along each child's 64 tiles the parent tile numbers rise strictly. `child_order`: one child has exactly 8192; every child has at least 4096.
All inputs are finite; a program needn't handle non-finite values.
Results may differ from the reference program's by a relative error of at most 0.0001.
Values sent between devices are 32-bit elements; how exact they have to be, the bound alone decides.
A program may use at most 128 MiB of HBM per device.

```python
import math
import jax
import jax.numpy as jnp
from jax import lax

B = 128
F = 12288
CB = 8192
NCH = 2
NPIV = 256
NT = 96
ROWS_GRID = 8
CT = 64
TRL = 8
NCD = 8
TCL = 8


def draw_parent_front(key, part):
    split_keys = jax.random.split(key, 3)
    noise_draw = jax.random.normal(split_keys[0], (F, F), jnp.float32)
    profile = jax.random.uniform(split_keys[1], (F,), jnp.float32, 0.5, 1.5)
    diagonal = jax.random.uniform(split_keys[2], (F,), jnp.float32, 16.0, 40.0)
    symmetric = (noise_draw + noise_draw.T) * (1.4142135 / math.sqrt(F))
    coherent = 0.25 * profile[:, None] * profile[None, :]
    numbers = jnp.arange(F, dtype=jnp.int32)
    on_diagonal = numbers[:, None] == numbers[None, :]
    return symmetric + coherent + jnp.where(on_diagonal, diagonal[None, :], 0.0)


def draw_child_blocks(key, part):
    within = jnp.arange(B, dtype=jnp.int32)
    numbers = jnp.arange(CT, dtype=jnp.int32)
    row_true = numbers % TRL * ROWS_GRID + numbers // TRL
    col_true = numbers % TCL * NCD + numbers // TCL
    row_pick = (row_true[:, None] * B + within[None, :]).reshape(-1)
    col_pick = (col_true[:, None] * B + within[None, :]).reshape(-1)
    blocks = []
    for child_number in range(NCH):
        child_key = jax.random.fold_in(key, child_number)
        split_keys = jax.random.split(child_key, 1)
        noise_draw = jax.random.normal(split_keys[0], (CB, CB), jnp.float32)
        symmetric = (noise_draw + noise_draw.T) * (1.4142135 / math.sqrt(CB))
        blocks.append(symmetric[row_pick][:, col_pick])
    return jnp.concatenate(blocks, axis=1)


def draw_child_map(key, part):
    steps_up = jax.random.randint(key, (NCH, CT), 0, 2)
    shifted = jnp.minimum(jnp.cumsum(steps_up, axis=1), NT - CT)
    numbers = jnp.arange(CT, dtype=jnp.int32)
    shifted = jnp.where(numbers[None, :] == CT - 1, NT - CT, shifted)
    shifted = jnp.where(numbers[None, :] == 0, 0, shifted)
    return (numbers[None, :] + shifted).astype(jnp.int32)


def draw_child_order(key, part):
    split_keys = jax.random.split(key, 2)
    order_draws = jax.random.randint(split_keys[0], (NCH,), CB // 2, CB + 1)
    fullest = jax.random.randint(split_keys[1], (), 0, NCH)
    return jnp.where(jnp.arange(NCH) == fullest, CB, order_draws).astype(jnp.int32)


def setup_inputs(seed: int = 0) -> dict:
    seeds = jax.random.split(jax.random.key(seed), 5)
    return {
        "parent_front": draw_parent_front(jax.random.fold_in(seeds[4], 71), 0),
        "child_blocks": draw_child_blocks(jax.random.fold_in(seeds[4], 71), 0),
        "child_map": draw_child_map(jax.random.fold_in(seeds[4], 71), 0),
        "child_order": draw_child_order(jax.random.fold_in(seeds[4], 71), 0),
    }


HIGHEST_PRECISION = lax.Precision.HIGHEST

def stored_positions(tile_total, group_count, per_group):
    numbers = jnp.arange(tile_total, dtype=jnp.int32)
    return numbers % group_count * per_group + numbers // group_count

def reference(parent_front, child_blocks, child_map, child_order):
    front_matrix = parent_front
    within = jnp.arange(B, dtype=jnp.int32)
    row_store = stored_positions(CT, ROWS_GRID, TRL)
    col_store = stored_positions(CT, NCD, TCL)
    row_pick = (row_store[:, None] * B + within[None, :]).reshape(-1)
    col_pick = (col_store[:, None] * B + within[None, :]).reshape(-1)
    for child_number in range(NCH):
        stored = child_blocks[:, child_number * CB:(child_number + 1) * CB]
        schur_block = stored[row_pick][:, col_pick]
        inside = jnp.arange(CB, dtype=jnp.int32) < child_order[child_number]
        schur_block = jnp.where(inside[:, None] & inside[None, :], schur_block, jnp.float32(0.0))
        positions = (child_map[child_number][:, None] * B + within[None, :]).reshape(-1)
        front_matrix = front_matrix.at[positions[:, None], positions[None, :]].add(schur_block)
    for panel_number in range(NPIV // B):
        panel_start = panel_number * B
        panel_end = panel_start + B
        factor = jnp.linalg.cholesky(front_matrix[panel_start:panel_end, panel_start:panel_end])
        below_rows = lax.linalg.triangular_solve(factor, front_matrix[panel_end:, panel_start:panel_end], left_side=False, lower=True, transpose_a=True)
        update = jnp.dot(below_rows.astype(jnp.float32), below_rows.T.astype(jnp.float32), precision=HIGHEST_PRECISION, preferred_element_type=jnp.float32)
        front_matrix = front_matrix.at[panel_end:, panel_end:].add(-update)
        front_matrix = front_matrix.at[:panel_start, panel_start:panel_end].set(jnp.float32(0.0))
        front_matrix = front_matrix.at[panel_start:panel_end, panel_start:panel_end].set(factor)
        front_matrix = front_matrix.at[panel_end:, panel_start:panel_end].set(below_rows)
    front_matrix = front_matrix.at[:NPIV, NPIV:].set(jnp.float32(0.0))
    return front_matrix
```

```python
import functools

import jax
import jax.numpy as jnp
from jax import lax
from jax.experimental import pallas as pl
from jax.experimental.pallas import tpu as pltpu
from jax.sharding import PartitionSpec as P

B = 128
NPIV = 256
ROWS = 8
COLS = 16
PARTS = 4
SUB = B // PARTS
MESH = pl.DeviceIdType.MESH
HI = lax.Precision.HIGHEST
VMEM_LIMIT = 66 * 1000 * 1000

T_INV = 0
T_SEL = 192
T_COL = 384
T_ROW = 640
T_ORD = 832
T_LEN = 834


def routing_table(child_map, child_order):
    kids, tiles = child_map.shape
    tile = jnp.arange(tiles, dtype=jnp.int32)
    place = jnp.arange(96, dtype=jnp.int32)
    hit = child_map[:, None, :] == place[None, :, None]
    inverse = jnp.sum(jnp.where(hit, tile[None, None, :] + 1, 0), axis=2) - 1
    window = child_map // 12
    same = (
        ((tile[:, None] - tile[None, :]) % ROWS == 0)
        & (tile[None, :] < tile[:, None])
    )
    rank = jnp.sum(
        (same[None] & (window[:, :, None] == window[:, None, :])).astype(jnp.int32), axis=2
    )
    slot = tile[None, :] % ROWS + ROWS * rank
    select = jnp.sum(jnp.where(hit, slot[:, None, :], 0), axis=2)
    grouped = child_map.reshape(kids, 8, 8)
    dest = jnp.arange(COLS, dtype=jnp.int32)
    step = jnp.arange(8, dtype=jnp.int32)
    col_pick = jnp.sum(
        jnp.where(
            (grouped // 6)[:, :, :, None] == dest[None, None, None, :],
            step[None, :, None, None],
            0,
        ),
        axis=1,
    )
    edges = jnp.arange(9, dtype=jnp.int32) * 12
    count = jnp.sum((grouped[:, :, :, None] < edges).astype(jnp.int32), axis=1)
    low, mid = count[:, :, 0:8:2], count[:, :, 1:9:2]
    extra = jnp.where(mid - low == 2, low + 1, mid + 1)
    row_pick = jnp.minimum(jnp.stack([low, mid, extra], axis=-1), 7)
    return jnp.concatenate(
        [
            inverse.reshape(-1),
            select.reshape(-1),
            col_pick.reshape(-1),
            row_pick.reshape(-1),
            child_order.reshape(-1),
        ]
    ).astype(jnp.int32)


def enter(row, col):
    barrier = pltpu.get_barrier_semaphore()
    for d in range(1, COLS):
        pl.semaphore_signal(
            barrier,
            inc=1,
            device_id={"col": lax.rem(col + d, COLS)},
            device_id_type=MESH,
        )
    for d in range(1, ROWS):
        pl.semaphore_signal(
            barrier,
            inc=1,
            device_id={"row": lax.rem(row + d, ROWS)},
            device_id_type=MESH,
        )
    pl.semaphore_wait(barrier, COLS + ROWS - 2)


def extend_kernel(tab, parent, child, out, kid_cols, load_sem, send_c, send_r, *rest):
    recv_c = rest[:PARTS]
    recv_r = rest[PARTS : 2 * PARTS]
    cs, cr, rs, dr, br, fs = rest[2 * PARTS :]
    row = lax.axis_index("row")
    col = lax.axis_index("col")
    chip = row // 2
    core = lax.rem(row, 2)
    other = 1 - core
    mate = row + 1 - 2 * core
    kid = col // 8
    slot = lax.rem(col, 8)
    loads = [
        pltpu.make_async_copy(
            child.at[:, k * B : (k + 1) * B], kid_cols.at[k], load_sem.at[k]
        )
        for k in range(8)
    ]
    for load in loads:
        load.start()
    enter(row, col)
    for load in loads:
        load.wait()

    def take_col(g, dest):
        k = tab[T_COL + (kid * 8 + slot) * COLS + dest]
        return [kid_cols[k, t * B + g * SUB : t * B + (g + 1) * SUB, :] for t in range(8)]

    def col_copy(g, d):
        dest = lax.rem(col + d, COLS)
        return pltpu.make_async_remote_copy(
            src_ref=send_c.at[g, dest],
            dst_ref=recv_c[g].at[col],
            send_sem=cs.at[g, d],
            recv_sem=cr.at[g, col],
            device_id={"col": dest},
            device_id_type=MESH,
        )

    def col_arrival(g, d):
        source = lax.rem(col + d, COLS)
        return pltpu.make_async_remote_copy(
            src_ref=send_c.at[g, source],
            dst_ref=recv_c[g].at[source],
            send_sem=cs.at[g, d],
            recv_sem=cr.at[g, source],
            device_id={"col": source},
            device_id_type=MESH,
        )

    for g in range(PARTS):

        @pl.loop(1, COLS)
        def _(d):
            dest = lax.rem(col + d, COLS)
            for t, piece in enumerate(take_col(g, dest)):
                send_c[g, dest, t] = piece

        for t, piece in enumerate(take_col(g, col)):
            recv_c[g][col, t] = piece

        @pl.loop(1, COLS)
        def _(d):
            col_copy(g, d).start()

    def direct_copy(g, dy, side):
        chip_to = lax.rem(chip + dy, 4)
        return pltpu.make_async_remote_copy(
            src_ref=send_r.at[g, chip_to * 3 + side],
            dst_ref=recv_r[g].at[row],
            send_sem=rs.at[g, dy * 3 + side],
            recv_sem=dr.at[g, row],
            device_id={"row": chip_to * 2 + side},
            device_id_type=MESH,
        )

    def mate_copy(g):
        return pltpu.make_async_remote_copy(
            src_ref=send_r.at[g, chip * 3 + other],
            dst_ref=recv_r[g].at[row],
            send_sem=rs.at[g, 0],
            recv_sem=dr.at[g, row],
            device_id={"row": mate},
            device_id_type=MESH,
        )

    def extra_copy(g, dy):
        chip_to = lax.rem(chip + dy, 4)
        return pltpu.make_async_remote_copy(
            src_ref=send_r.at[g, chip_to * 3 + 2],
            dst_ref=recv_r[g].at[8 + row],
            send_sem=rs.at[g, dy * 3 + 2],
            recv_sem=br.at[g, row],
            device_id={"row": chip_to * 2 + core},
            device_id_type=MESH,
        )

    def row_arrival(g, source, base, sem):
        return pltpu.make_async_remote_copy(
            src_ref=send_r.at[g, 0],
            dst_ref=recv_r[g].at[base + source],
            send_sem=rs.at[g, 0],
            recv_sem=sem.at[g, source],
            device_id={"row": source},
            device_id_type=MESH,
        )

    def forward_copy(g, dy):
        source = lax.rem(chip + dy, 4) * 2 + core
        return pltpu.make_async_remote_copy(
            src_ref=recv_r[g].at[8 + source],
            dst_ref=recv_r[g].at[8 + source],
            send_sem=fs.at[g, dy],
            recv_sem=br.at[g, source],
            device_id={"row": mate},
            device_id_type=MESH,
        )

    def spread_rows(g):
        @pl.loop(1, COLS)
        def _(d):
            col_arrival(g, d).wait_recv()

        sources = []
        for h in range(2):
            for b in range(6):
                j = jnp.maximum(tab[T_INV + h * 96 + col * 6 + b], 0)
                sources.append(h * 8 + lax.rem(j, 8))

        @pl.loop(0, 12)
        def _(q):
            for h in range(2):
                k = tab[T_ROW + (h * 8 + row) * 12 + q]
                for b in range(6):
                    send_r[g, q, h, :, b * B : (b + 1) * B] = recv_c[g][sources[h * 6 + b], k]

        recv_r[g][row] = send_r[g, chip * 3 + core]
        recv_r[g][8 + row] = send_r[g, chip * 3 + 2]
        for dy in (2, 1, 3):
            direct_copy(g, dy, 0).start()
            direct_copy(g, dy, 1).start()
            extra_copy(g, dy).start()
        mate_copy(g).start()
        forward_copy(g, 0).start()

    def forward(g):
        for dy in range(1, 4):
            row_arrival(g, lax.rem(chip + dy, 4) * 2 + core, 8, br).wait_recv()
            forward_copy(g, dy).start()

    def land(g):
        for d in range(1, ROWS):
            row_arrival(g, lax.rem(row + d, ROWS), 0, dr).wait_recv()
        for dy in range(4):
            row_arrival(g, lax.rem(chip + dy, 4) * 2 + other, 8, br).wait_recv()
        lane = lax.broadcasted_iota(jnp.int32, (1, B), 1)
        alive = []
        for h in range(2):
            order = tab[T_ORD + h]
            for b in range(6):
                j = tab[T_INV + h * 96 + col * 6 + b]
                limit = jnp.where(j < 0, 0, order - j * B)
                alive.append(lane < limit)
        down = lax.broadcasted_iota(jnp.int32, (SUB, 1), 0) + g * SUB

        @pl.loop(0, 12)
        def _(a):
            start = pl.multiple_of(a * B + g * SUB, SUB)
            picks, lives = [], []
            for h in range(2):
                place = h * 96 + row * 12 + a
                i = tab[T_INV + place]
                limit = jnp.where(i < 0, 0, tab[T_ORD + h] - i * B)
                picks.append(tab[T_SEL + place])
                lives.append(down < limit)
            for b in range(6):
                span = slice(b * B, (b + 1) * B)
                total = parent[pl.ds(start, SUB), span]
                for h in range(2):
                    piece = recv_r[g][picks[h], h, :, span]
                    total = total + jnp.where(lives[h] & alive[h * 6 + b], piece, 0.0)
                out[pl.ds(start, SUB), span] = total

    for g in range(PARTS):
        spread_rows(g)
        if g >= 1:
            forward(g - 1)
        if g >= 2:
            land(g - 2)
    forward(PARTS - 1)
    for g in range(max(PARTS - 2, 0), PARTS):
        land(g)

    for g in range(PARTS):

        @pl.loop(1, COLS)
        def _(d):
            col_copy(g, d).wait_send()

        for dy in range(1, 4):
            direct_copy(g, dy, 0).wait_send()
            direct_copy(g, dy, 1).wait_send()
            extra_copy(g, dy).wait_send()
        mate_copy(g).wait_send()
        for dy in range(4):
            forward_copy(g, dy).wait_send()


def mul(a, b, ca, cb):
    return lax.dot_general(
        a,
        b,
        (((ca,), (cb,)), ((), ())),
        precision=HI,
        preferred_element_type=jnp.float32,
    )


def eliminate(work):
    wide = lax.broadcasted_iota(jnp.int32, (B, B), 1)
    tall = lax.broadcasted_iota(jnp.int32, (B, B), 0)
    one = lax.broadcasted_iota(jnp.int32, (1, B), 1)
    down = lax.broadcasted_iota(jnp.int32, (B, 1), 0)

    def body(j, carry):
        pivot_row = work[pl.ds(j, 1), :]
        pivot = jnp.sum(jnp.where(one == j, pivot_row[:, :B], 0.0), axis=1, keepdims=True)
        column = jnp.sum(jnp.where(wide == j, work[:, :B], 0.0), axis=1, keepdims=True)
        factor = jnp.where(down > j, column / pivot, 0.0)
        work[...] = work[...] - factor * pivot_row
        return carry

    lax.fori_loop(0, B - 1, body, 0)
    upper = work[:, :B]
    diagonal = jnp.sum(jnp.where(wide == tall, upper, 0.0), axis=1, keepdims=True)
    scale = lax.rsqrt(diagonal)
    scale = scale * (1.5 - 0.5 * diagonal * scale * scale)
    upper_factor = jnp.where(wide >= tall, upper * scale, 0.0)
    inverse = jnp.where(wide <= tall, work[:, B:] * scale, 0.0)
    return upper_factor, inverse


def factor_kernel(
    front, out, corner, mine, rows_ref, work, lower, inv, left, right, s_a, r_a, s_u, r_u, s_p, r_p
):
    row = lax.axis_index("row")
    col = lax.axis_index("col")
    chip = row // 2
    core = lax.rem(row, 2)
    zed = col // 4
    ex = lax.rem(col, 4)
    enter(row, col)

    def copy(src, dst, send, recv, **where):
        return pltpu.make_async_remote_copy(
            src_ref=src,
            dst_ref=dst,
            send_sem=send,
            recv_sem=recv,
            device_id=where,
            device_id_type=MESH,
        )

    def corner_copy(index, **where):
        return copy(corner, corner, s_a.at[index], r_a, **where)

    def mine_copy(index, **where):
        return copy(mine, mine, s_u.at[index], r_u, **where)

    piece = lax.rem(ex, 2)

    def z_copy(d):
        to = lax.rem(zed + d, 4) * 4 + ex
        return copy(mine, rows_ref.at[piece], s_p.at[d - 1], r_p.at[piece], col=to)

    def x_copy(d):
        to = zed * 4 + lax.rem(ex + d, 4)
        return copy(
            rows_ref.at[piece], rows_ref.at[piece], s_p.at[2 + d], r_p.at[piece], col=to
        )

    def piece_arrival(index):
        return copy(mine, rows_ref.at[index], s_p.at[0], r_p.at[index], col=col)

    owner = col // 2 == row
    holder = ex // 2 == core
    top = row == 0
    first = top & (col == 0)
    relay = (core == 0) & (row > 0)

    @pl.when(top)
    def _():
        mine[...] = front[0:NPIV, :]

    @pl.when(first)
    def _():
        corner[...] = front[0:NPIV, 0:NPIV]
        for d in (2, 8, 1, 3, 4, 12, 5, 6, 7, 9, 10, 11, 13, 14, 15):
            corner_copy(d, col=d).start()

    @pl.when(jnp.logical_not(first))
    def _():
        corner_copy(0, col=col).wait_recv()

    @pl.when(top)
    def _():
        for d in (4, 2, 6, 1):
            corner_copy(15 + d, row=d).start()
        for d in (4, 2, 6, 1):
            mine_copy(d, row=d).start()

    @pl.when(relay)
    def _():
        corner_copy(16, row=row + 1).start()

    work[:, :B] = corner[:B, :B]
    tall = lax.broadcasted_iota(jnp.int32, (B, B), 0)
    wide = lax.broadcasted_iota(jnp.int32, (B, B), 1)
    unit = (tall == wide).astype(jnp.float32)
    work[:, B:] = unit
    up1, inv1 = eliminate(work)
    low21 = mul(corner[B:, :B], inv1, 1, 1)
    inv[:B, :B] = inv1
    inv[:B, B:] = jnp.zeros((B, B), jnp.float32)
    lower[:B, :B] = up1.T
    lower[:B, B:] = jnp.zeros((B, B), jnp.float32)
    lower[B:, :B] = low21

    @pl.when(jnp.logical_not(top))
    def _():
        mine_copy(0, row=row).wait_recv()

    @pl.when(relay)
    def _():
        mine_copy(1, row=row + 1).start()

    @pl.when(owner)
    def _():
        for d in (2, 1, 3):
            z_copy(d).start()
        rows_ref[piece] = mine[...]

    work[:, :B] = corner[B:, B:] - mul(low21, low21, 1, 1)
    work[:, B:] = unit
    up2, inv2 = eliminate(work)
    inv[B:, B:] = inv2
    inv[B:, :B] = -mul(inv2, mul(lower[B:, :B], inv[:B, :B], 1, 0), 1, 0)
    lower[B:, B:] = up2.T

    @pl.when(holder)
    def _():
        @pl.when(jnp.logical_not(owner))
        def _():
            piece_arrival(piece).wait_recv()

        for d in (2, 1, 3):
            x_copy(d).start()

    right[...] = mul(inv[...], mine[...], 1, 0)

    @pl.when(jnp.logical_not(holder & (piece == 0)))
    def _():
        piece_arrival(0).wait_recv()

    left[0] = mul(inv[...], rows_ref[0], 1, 0)

    @pl.when(jnp.logical_not(holder & (piece == 1)))
    def _():
        piece_arrival(1).wait_recv()

    left[1] = mul(inv[...], rows_ref[1], 1, 0)

    @pl.loop(0, 6)
    def _(n):
        block = left[n // 3, :, pl.ds(pl.multiple_of(lax.rem(n, 3) * NPIV, NPIV), NPIV)]
        here = pl.ds(pl.multiple_of(n * NPIV, NPIV), NPIV)
        out[here, :] = front[here, :] - mul(block, right[...], 0, 0)

        @pl.when(col == 0)
        def _():
            out[here, 0:NPIV] = block.T

    @pl.when(top)
    def _():
        out[0:NPIV, :] = jnp.zeros((NPIV, out.shape[1]), jnp.float32)

    @pl.when(first)
    def _():
        out[0:NPIV, 0:NPIV] = lower[...]

    @pl.when(first)
    def _():
        for d in range(1, COLS):
            corner_copy(d, col=d).wait_send()

    @pl.when(top)
    def _():
        for d in (4, 2, 6, 1):
            corner_copy(15 + d, row=d).wait_send()
        for d in (4, 2, 6, 1):
            mine_copy(d, row=d).wait_send()

    @pl.when(relay)
    def _():
        corner_copy(16, row=row + 1).wait_send()
        mine_copy(1, row=row + 1).wait_send()

    @pl.when(owner)
    def _():
        for d in (2, 1, 3):
            z_copy(d).wait_send()

    @pl.when(holder)
    def _():
        for d in (2, 1, 3):
            x_copy(d).wait_send()


def shards(parent_front, child_blocks, child_map, child_order):
    table = routing_table(child_map, child_order)
    shape = jax.ShapeDtypeStruct(parent_front.shape, jnp.float32)
    vmem = pl.BlockSpec(memory_space=pltpu.VMEM)
    width = parent_front.shape[1]
    front = pl.pallas_call(
        extend_kernel,
        out_shape=shape,
        in_specs=[
            pl.BlockSpec(memory_space=pltpu.SMEM),
            vmem,
            pl.BlockSpec(memory_space=pl.ANY),
        ],
        out_specs=vmem,
        scratch_shapes=[
            pltpu.VMEM((8, 8 * B, B), jnp.float32),
            pltpu.SemaphoreType.DMA((8,)),
            pltpu.VMEM((PARTS, COLS, 8, SUB, B), jnp.float32),
            pltpu.VMEM((PARTS, 12, 2, SUB, width), jnp.float32),
        ]
        + [pltpu.VMEM((COLS, 8, SUB, B), jnp.float32)] * PARTS
        + [pltpu.VMEM((16, 2, SUB, width), jnp.float32)] * PARTS
        + [
            pltpu.SemaphoreType.DMA((PARTS, COLS)),
            pltpu.SemaphoreType.DMA((PARTS, COLS)),
            pltpu.SemaphoreType.DMA((PARTS, 12)),
            pltpu.SemaphoreType.DMA((PARTS, ROWS)),
            pltpu.SemaphoreType.DMA((PARTS, ROWS)),
            pltpu.SemaphoreType.DMA((PARTS, 4)),
        ],
        compiler_params=pltpu.CompilerParams(
            collective_id=0, has_side_effects=True, vmem_limit_bytes=VMEM_LIMIT
        ),
        name="extend_add",
    )(table, parent_front, child_blocks)
    return pl.pallas_call(
        factor_kernel,
        out_shape=shape,
        in_specs=[vmem],
        out_specs=vmem,
        scratch_shapes=[
            pltpu.VMEM((NPIV, NPIV), jnp.float32),
            pltpu.VMEM((NPIV, width), jnp.float32),
            pltpu.VMEM((2, NPIV, width), jnp.float32),
            pltpu.VMEM((B, 2 * B), jnp.float32),
            pltpu.VMEM((NPIV, NPIV), jnp.float32),
            pltpu.VMEM((NPIV, NPIV), jnp.float32),
            pltpu.VMEM((2, NPIV, width), jnp.float32),
            pltpu.VMEM((NPIV, width), jnp.float32),
            pltpu.SemaphoreType.DMA((24,)),
            pltpu.SemaphoreType.DMA,
            pltpu.SemaphoreType.DMA((8,)),
            pltpu.SemaphoreType.DMA,
            pltpu.SemaphoreType.DMA((6,)),
            pltpu.SemaphoreType.DMA((2,)),
        ],
        compiler_params=pltpu.CompilerParams(
            collective_id=1, has_side_effects=True, vmem_limit_bytes=VMEM_LIMIT
        ),
        name="factor",
    )(front)


def solution(mesh):
    placed = (P("row", "col"), P("row", "col"), P(), P())
    return jax.shard_map(
        shards, mesh=mesh, in_specs=placed, out_specs=P("row", "col"), check_vma=False
    )
```

```python
import functools

import jax
import jax.numpy as jnp
from jax import lax
from jax.experimental import pallas as pl
from jax.experimental.pallas import tpu as pltpu
from jax.sharding import PartitionSpec as P

B = 128
NPIV = 256
ROWS = 8
COLS = 16
PARTS = 8
SUB = B // PARTS
MESH = pl.DeviceIdType.MESH
HI = lax.Precision.HIGHEST
VMEM_LIMIT = 66 * 1000 * 1000

T_INV = 0
T_SEL = 192
T_COL = 384
T_ROW = 640
T_ORD = 832
T_LEN = 834


def routing_table(child_map, child_order):
    kids, tiles = child_map.shape
    tile = jnp.arange(tiles, dtype=jnp.int32)
    place = jnp.arange(96, dtype=jnp.int32)
    hit = child_map[:, None, :] == place[None, :, None]
    inverse = jnp.sum(jnp.where(hit, tile[None, None, :] + 1, 0), axis=2) - 1
    window = child_map // 12
    same = (
        ((tile[:, None] - tile[None, :]) % ROWS == 0)
        & (tile[None, :] < tile[:, None])
    )
    rank = jnp.sum(
        (same[None] & (window[:, :, None] == window[:, None, :])).astype(jnp.int32), axis=2
    )
    slot = tile[None, :] % ROWS + ROWS * rank
    select = jnp.sum(jnp.where(hit, slot[:, None, :], 0), axis=2)
    grouped = child_map.reshape(kids, 8, 8)
    dest = jnp.arange(COLS, dtype=jnp.int32)
    step = jnp.arange(8, dtype=jnp.int32)
    col_pick = jnp.sum(
        jnp.where(
            (grouped // 6)[:, :, :, None] == dest[None, None, None, :],
            step[None, :, None, None],
            0,
        ),
        axis=1,
    )
    edges = jnp.arange(9, dtype=jnp.int32) * 12
    count = jnp.sum((grouped[:, :, :, None] < edges).astype(jnp.int32), axis=1)
    low, mid = count[:, :, 0:8:2], count[:, :, 1:9:2]
    extra = jnp.where(mid - low == 2, low + 1, mid + 1)
    row_pick = jnp.minimum(jnp.stack([low, mid, extra], axis=-1), 7)
    return jnp.concatenate(
        [
            inverse.reshape(-1),
            select.reshape(-1),
            col_pick.reshape(-1),
            row_pick.reshape(-1),
            child_order.reshape(-1),
        ]
    ).astype(jnp.int32)


def enter(row, col):
    barrier = pltpu.get_barrier_semaphore()
    for d in range(1, COLS):
        pl.semaphore_signal(
            barrier,
            inc=1,
            device_id={"col": lax.rem(col + d, COLS)},
            device_id_type=MESH,
        )
    for d in range(1, ROWS):
        pl.semaphore_signal(
            barrier,
            inc=1,
            device_id={"row": lax.rem(row + d, ROWS)},
            device_id_type=MESH,
        )
    pl.semaphore_wait(barrier, COLS + ROWS - 2)


def mul(a, b, ca, cb):
    return lax.dot_general(
        a,
        b,
        (((ca,), (cb,)), ((), ())),
        precision=HI,
        preferred_element_type=jnp.float32,
    )


def eliminate(work, first, last):
    wide = lax.broadcasted_iota(jnp.int32, (B, B), 1)
    one = lax.broadcasted_iota(jnp.int32, (1, B), 1)
    down = lax.broadcasted_iota(jnp.int32, (B, 1), 0)

    def body(j, carry):
        pivot_row = work[pl.ds(j, 1), :]
        pivot = jnp.sum(jnp.where(one == j, pivot_row[:, :B], 0.0), axis=1, keepdims=True)
        column = jnp.sum(jnp.where(wide == j, work[:, :B], 0.0), axis=1, keepdims=True)
        factor = jnp.where(down > j, column * (1.0 / pivot), 0.0)
        work[...] = work[...] - factor * pivot_row
        return carry

    lax.fori_loop(first, last, body, 0)


def eliminated(work):
    wide = lax.broadcasted_iota(jnp.int32, (B, B), 1)
    tall = lax.broadcasted_iota(jnp.int32, (B, B), 0)
    upper = work[:, :B]
    diagonal = jnp.sum(jnp.where(wide == tall, upper, 0.0), axis=1, keepdims=True)
    scale = lax.rsqrt(diagonal)
    scale = scale * (1.5 - 0.5 * diagonal * scale * scale)
    upper_factor = jnp.where(wide >= tall, upper * scale, 0.0)
    inverse = jnp.where(wide <= tall, work[:, B:] * scale, 0.0)
    return upper_factor, inverse


def front_kernel(
    tab,
    parent,
    child,
    out,
    kid_cols,
    send_c,
    send_r,
    send_p,
    recv_p,
    late,
    corner,
    mine,
    rows_ref,
    work,
    lower,
    inv,
    left,
    right,
    load_sem,
    cs,
    cr,
    rs,
    dr,
    br,
    fs,
    ps,
    pr,
    s_a,
    s_u,
    s_p,
    r_p,
    misc,
    *rest,
):
    recv_c = rest[:PARTS]
    recv_r = rest[PARTS:]
    row = lax.axis_index("row")
    col = lax.axis_index("col")
    chip = row // 2
    core = lax.rem(row, 2)
    other = 1 - core
    mate = row + 1 - 2 * core
    kid = col // 8
    slot = lax.rem(col, 8)
    zed = col // 4
    ex = lax.rem(col, 4)
    piece = lax.rem(ex, 2)
    owner = col // 2 == row
    holder = ex // 2 == core
    top = row == 0
    first = top & (col == 0)
    relay = (core == 0) & (row > 0)
    loads = [
        pltpu.make_async_copy(
            child.at[:, k * B : (k + 1) * B], kid_cols.at[k], load_sem.at[k]
        )
        for k in range(8)
    ]
    loads.append(pltpu.make_async_copy(parent, out, load_sem.at[8]))
    for load in loads:
        load.start()
    enter(row, col)
    for load in loads:
        load.wait()

    def copy(src, dst, send, recv, **where):
        return pltpu.make_async_remote_copy(
            src_ref=src,
            dst_ref=dst,
            send_sem=send,
            recv_sem=recv,
            device_id=where,
            device_id_type=MESH,
        )

    def pick_col(dest):
        return tab[T_COL + (kid * 8 + slot) * COLS + dest]

    def take_col(g, dest):
        k = pick_col(dest)
        return [kid_cols[k, t * B + g * SUB : t * B + (g + 1) * SUB, :] for t in range(8)]

    def col_copy(g, d):
        dest = lax.rem(col + d, COLS)
        return copy(
            send_c.at[g, dest], recv_c[g].at[col], cs.at[g, d], cr.at[g, col], col=dest
        )

    def col_arrival(g, d):
        source = lax.rem(col + d, COLS)
        return copy(
            send_c.at[g, source], recv_c[g].at[source], cs.at[g, d], cr.at[g, source], col=source
        )

    def pack_cols(g):
        @pl.loop(1, COLS)
        def _(d):
            dest = lax.rem(col + d, COLS)
            for t, part in enumerate(take_col(g, dest)):
                send_c[g, dest, t] = part

        for t, part in enumerate(take_col(g, col)):
            recv_c[g][col, t] = part

    def send_cols(g):
        @pl.loop(1, COLS)
        def _(d):
            col_copy(g, d).start()

    def panel_copy(d):
        dest = lax.rem(col + d, COLS)
        return copy(send_p.at[dest], recv_p.at[col], ps.at[d], pr.at[col], col=dest)

    def panel_arrival(d):
        source = lax.rem(col + d, COLS)
        return copy(send_p.at[source], recv_p.at[source], ps.at[d], pr.at[source], col=source)

    def late_copy():
        return copy(late, late, misc.at[0], misc.at[1], row=0)

    def late_arrival():
        return copy(late, late, misc.at[0], misc.at[1], row=1)

    def corner_copy(index, **where):
        return copy(corner, corner, s_a.at[index], misc.at[2], **where)

    def mine_copy(index, **where):
        return copy(mine, mine, s_u.at[index], misc.at[3], **where)

    def z_copy(d):
        to = lax.rem(zed + d, 4) * 4 + ex
        return copy(mine, rows_ref.at[piece], s_p.at[d - 1], r_p.at[piece], col=to)

    def x_copy(d):
        to = zed * 4 + lax.rem(ex + d, 4)
        return copy(
            rows_ref.at[piece], rows_ref.at[piece], s_p.at[2 + d], r_p.at[piece], col=to
        )

    def piece_arrival(index):
        return copy(mine, rows_ref.at[index], s_p.at[0], r_p.at[index], col=col)

    pack_cols(0)
    send_cols(0)

    @pl.when(row < 2)
    def _():
        @pl.loop(1, COLS)
        def _(d):
            dest = lax.rem(col + d, COLS)
            send_p[dest] = kid_cols[pick_col(dest), 0:B, :]

        recv_p[col] = kid_cols[pick_col(col), 0:B, :]

        @pl.loop(1, COLS)
        def _(d):
            panel_copy(d).start()

    pack_cols(1)
    send_cols(1)
    for g in range(2, PARTS):
        pack_cols(g)

    def direct_copy(g, dy, side):
        chip_to = lax.rem(chip + dy, 4)
        return copy(
            send_r.at[g, chip_to * 3 + side],
            recv_r[g].at[row],
            rs.at[g, dy * 3 + side],
            dr.at[g, row],
            row=chip_to * 2 + side,
        )

    def mate_copy(g):
        return copy(
            send_r.at[g, chip * 3 + other], recv_r[g].at[row], rs.at[g, 0], dr.at[g, row], row=mate
        )

    def extra_copy(g, dy):
        chip_to = lax.rem(chip + dy, 4)
        return copy(
            send_r.at[g, chip_to * 3 + 2],
            recv_r[g].at[8 + row],
            rs.at[g, dy * 3 + 2],
            br.at[g, row],
            row=chip_to * 2 + core,
        )

    def row_arrival(g, source, base, sem):
        return copy(
            send_r.at[g, 0], recv_r[g].at[base + source], rs.at[g, 0], sem.at[g, source], row=source
        )

    def forward_copy(g, dy):
        source = lax.rem(chip + dy, 4) * 2 + core
        return copy(
            recv_r[g].at[8 + source],
            recv_r[g].at[8 + source],
            fs.at[g, dy],
            br.at[g, source],
            row=mate,
        )

    def spread_rows(g):
        @pl.loop(1, COLS)
        def _(d):
            col_arrival(g, d).wait_recv()

        sources = []
        for h in range(2):
            for b in range(6):
                j = jnp.maximum(tab[T_INV + h * 96 + col * 6 + b], 0)
                sources.append(h * 8 + lax.rem(j, 8))

        @pl.loop(0, 12)
        def _(q):
            for h in range(2):
                k = tab[T_ROW + (h * 8 + row) * 12 + q]
                for b in range(6):
                    send_r[g, q, h, :, b * B : (b + 1) * B] = recv_c[g][sources[h * 6 + b], k]

        recv_r[g][row] = send_r[g, chip * 3 + core]
        recv_r[g][8 + row] = send_r[g, chip * 3 + 2]
        for dy in (2, 1, 3):
            extra_copy(g, dy).start()
            direct_copy(g, dy, 0).start()
            direct_copy(g, dy, 1).start()
        mate_copy(g).start()
        forward_copy(g, 0).start()

    def forward(g):
        for dy in range(1, 4):
            row_arrival(g, lax.rem(chip + dy, 4) * 2 + core, 8, br).wait_recv()
            forward_copy(g, dy).start()

    lane = lax.broadcasted_iota(jnp.int32, (1, B), 1)

    def land(g):
        for d in range(1, ROWS):
            row_arrival(g, lax.rem(row + d, ROWS), 0, dr).wait_recv()
        for dy in range(4):
            row_arrival(g, lax.rem(chip + dy, 4) * 2 + other, 8, br).wait_recv()
        alive = []
        for h in range(2):
            for b in range(6):
                j = tab[T_INV + h * 96 + col * 6 + b]
                limit = jnp.where(j < 0, 0, tab[T_ORD + h] - j * B)
                if b < 2:
                    limit = jnp.where(col == 0, 0, limit)
                alive.append(lane < limit)
        down = lax.broadcasted_iota(jnp.int32, (SUB, 1), 0) + g * SUB

        @pl.loop(0, 12)
        def _(a):
            start = pl.multiple_of(a * B + g * SUB, SUB)
            picks, lives = [], []
            for h in range(2):
                place = h * 96 + row * 12 + a
                i = tab[T_INV + place]
                limit = jnp.where(i < 0, 0, tab[T_ORD + h] - i * B)
                limit = jnp.where(row * 12 + a < 2, 0, limit)
                picks.append(tab[T_SEL + place])
                lives.append(down < limit)
            for b in range(6):
                span = slice(b * B, (b + 1) * B)
                total = out[pl.ds(start, SUB), span]
                for h in range(2):
                    part = recv_r[g][picks[h], h, :, span]
                    total = total + jnp.where(lives[h] & alive[h * 6 + b], part, 0.0)
                out[pl.ds(start, SUB), span] = total

    def frame(place, who, b):
        total = jnp.zeros((B, B), jnp.float32)
        for h in range(2):
            j = tab[T_INV + h * 96 + col * 6 + b]
            source = h * 8 + lax.rem(jnp.maximum(j, 0), 8)
            limit = jnp.where(j < 0, 0, tab[T_ORD + h] - j * B)
            limit = jnp.where(tab[T_INV + h * 96 + place] == who, limit, 0)
            total = total + jnp.where(lane < limit, recv_p[source], 0.0)
        return total

    tall = lax.broadcasted_iota(jnp.int32, (B, B), 0)
    wide = lax.broadcasted_iota(jnp.int32, (B, B), 1)

    def gather_panel():
        @pl.when(row < 2)
        def _():
            @pl.loop(1, COLS)
            def _(d):
                panel_arrival(d).wait_recv()

        @pl.when(row == 1)
        def _():
            for b in range(6):
                late[:, b * B : (b + 1) * B] = frame(1, 1, b)
            late_copy().start()

        @pl.when(top)
        def _():
            for place in range(2):
                here = slice(place * B, (place + 1) * B)
                for b in range(6):
                    span = slice(b * B, (b + 1) * B)
                    mine[here, span] = out[here, span] + frame(place, 0, b)
            late_arrival().wait_recv()
            mine[B:, :] = mine[B:, :] + late[...]

        @pl.when(first)
        def _():
            corner[...] = mine[:, 0:NPIV]
            for d in (2, 8, 1, 3, 4, 12, 5, 6, 7, 9, 10, 11, 13, 14, 15):
                corner_copy(d, col=d).start()

    def spread_panel():
        @pl.when(top & jnp.logical_not(first))
        def _():
            corner_copy(0, col=col).wait_recv()

        @pl.when(top)
        def _():
            for d in (4, 2, 6, 1):
                corner_copy(15 + d, row=d).start()
            for d in (4, 2, 6, 1):
                mine_copy(d, row=d).start()

    def relay_corner():
        @pl.when(relay)
        def _():
            corner_copy(0, row=row).wait_recv()
            corner_copy(16, row=row + 1).start()

    def begin_factor():
        @pl.when(core == 1)
        def _():
            corner_copy(0, row=row).wait_recv()

        work[:, :B] = corner[:B, :B]
        work[:, B:] = (tall == wide).astype(jnp.float32)
        eliminate(work, 0, 64)

    def share_mine():
        @pl.when(owner)
        def _():
            for d in (2, 1, 3):
                z_copy(d).start()
            rows_ref[piece] = mine[...]

    def half_factor():
        @pl.when(relay)
        def _():
            mine_copy(0, row=row).wait_recv()
            mine_copy(1, row=row + 1).start()

        @pl.when(core == 0)
        def _():
            share_mine()

        eliminate(work, 64, B - 1)
        up, low_inv = eliminated(work)
        low21 = mul(corner[B:, :B], low_inv, 1, 1)
        inv[:B, :B] = low_inv
        inv[:B, B:] = jnp.zeros((B, B), jnp.float32)
        lower[:B, :B] = up.T
        lower[:B, B:] = jnp.zeros((B, B), jnp.float32)
        lower[B:, :B] = low21
        work[:, :B] = corner[B:, B:] - mul(low21, low21, 1, 1)
        work[:, B:] = (tall == wide).astype(jnp.float32)

    def late_factor():
        @pl.when(core == 1)
        def _():
            mine_copy(0, row=row).wait_recv()
            share_mine()

        eliminate(work, 0, 64)

    def end_factor():
        @pl.when(holder)
        def _():
            @pl.when(jnp.logical_not(owner))
            def _():
                piece_arrival(piece).wait_recv()

            for d in (2, 1, 3):
                x_copy(d).start()

        eliminate(work, 64, B - 1)
        up, low_inv = eliminated(work)
        inv[B:, B:] = low_inv
        inv[B:, :B] = -mul(low_inv, mul(lower[B:, :B], inv[:B, :B], 1, 0), 1, 0)
        lower[B:, B:] = up.T

    def solve_own():
        right[...] = mul(inv[...], mine[...], 1, 0)

    def solve_rows():
        for index in range(2):

            @pl.when(jnp.logical_not(holder & (piece == index)))
            def _():
                piece_arrival(index).wait_recv()

            left[index] = mul(inv[...], rows_ref[index], 1, 0)

    def update():
        @pl.loop(0, 6)
        def _(n):
            block = left[n // 3, :, pl.ds(pl.multiple_of(lax.rem(n, 3) * NPIV, NPIV), NPIV)]
            here = pl.ds(pl.multiple_of(n * NPIV, NPIV), NPIV)
            out[here, :] = out[here, :] - mul(block, right[...], 0, 0)

            @pl.when(col == 0)
            def _():
                out[here, 0:NPIV] = block.T

        @pl.when(top)
        def _():
            out[0:NPIV, :] = jnp.zeros((NPIV, out.shape[1]), jnp.float32)

        @pl.when(first)
        def _():
            out[0:NPIV, 0:NPIV] = lower[...]

    hooks = [
        gather_panel,
        spread_panel,
        relay_corner,
        begin_factor,
        half_factor,
        late_factor,
        end_factor,
        solve_own,
    ]
    for g in range(PARTS):
        if g + 2 < PARTS:
            send_cols(g + 2)
        spread_rows(g)
        if g >= 1:
            forward(g - 1)
        if g >= 2:
            land(g - 2)
        hooks[g]()
    solve_rows()
    forward(PARTS - 1)
    land(PARTS - 2)
    update()
    land(PARTS - 1)

    for g in range(PARTS):

        @pl.loop(1, COLS)
        def _(d):
            col_copy(g, d).wait_send()

        for dy in range(1, 4):
            direct_copy(g, dy, 0).wait_send()
            direct_copy(g, dy, 1).wait_send()
            extra_copy(g, dy).wait_send()
        mate_copy(g).wait_send()
        for dy in range(4):
            forward_copy(g, dy).wait_send()

    @pl.when(row < 2)
    def _():
        @pl.loop(1, COLS)
        def _(d):
            panel_copy(d).wait_send()

    @pl.when(row == 1)
    def _():
        late_copy().wait_send()

    @pl.when(first)
    def _():
        for d in range(1, COLS):
            corner_copy(d, col=d).wait_send()

    @pl.when(top)
    def _():
        for d in (4, 2, 6, 1):
            corner_copy(15 + d, row=d).wait_send()
            mine_copy(d, row=d).wait_send()

    @pl.when(relay)
    def _():
        corner_copy(16, row=row + 1).wait_send()
        mine_copy(1, row=row + 1).wait_send()

    @pl.when(owner)
    def _():
        for d in (2, 1, 3):
            z_copy(d).wait_send()

    @pl.when(holder)
    def _():
        for d in (2, 1, 3):
            x_copy(d).wait_send()


def shards(parent_front, child_blocks, child_map, child_order):
    table = routing_table(child_map, child_order)
    width = parent_front.shape[1]
    wild = pl.BlockSpec(memory_space=pl.ANY)

    def vmem(*shape):
        return pltpu.VMEM(shape, jnp.float32)

    dma = pltpu.SemaphoreType.DMA
    return pl.pallas_call(
        front_kernel,
        out_shape=jax.ShapeDtypeStruct(parent_front.shape, jnp.float32),
        in_specs=[pl.BlockSpec(memory_space=pltpu.SMEM), wild, wild],
        out_specs=pl.BlockSpec(memory_space=pltpu.VMEM),
        scratch_shapes=[
            vmem(8, 8 * B, B),
            vmem(PARTS, COLS, 8, SUB, B),
            vmem(PARTS, 12, 2, SUB, width),
            vmem(COLS, B, B),
            vmem(COLS, B, B),
            vmem(B, width),
            vmem(NPIV, NPIV),
            vmem(NPIV, width),
            vmem(2, NPIV, width),
            vmem(B, 2 * B),
            vmem(NPIV, NPIV),
            vmem(NPIV, NPIV),
            vmem(2, NPIV, width),
            vmem(NPIV, width),
            dma((9,)),
            dma((PARTS, COLS)),
            dma((PARTS, COLS)),
            dma((PARTS, 12)),
            dma((PARTS, ROWS)),
            dma((PARTS, ROWS)),
            dma((PARTS, 4)),
            dma((COLS,)),
            dma((COLS,)),
            dma((24,)),
            dma((8,)),
            dma((6,)),
            dma((2,)),
            dma((4,)),
        ]
        + [vmem(COLS, 8, SUB, B)] * PARTS
        + [vmem(16, 2, SUB, width)] * PARTS,
        compiler_params=pltpu.CompilerParams(
            collective_id=0, has_side_effects=True, vmem_limit_bytes=VMEM_LIMIT
        ),
        name="front",
    )(table, parent_front, child_blocks)


def solution(mesh):
    placed = (P("row", "col"), P("row", "col"), P(), P())
    return jax.shard_map(
        shards, mesh=mesh, in_specs=placed, out_specs=P("row", "col"), check_vma=False
    )
```

```python
import functools

import jax
import jax.numpy as jnp
from jax import lax
from jax.experimental import pallas as pl
from jax.experimental.pallas import tpu as pltpu
from jax.sharding import PartitionSpec as P

B = 128
NPIV = 256
ROWS = 8
COLS = 16
PARTS = 8
Z_EVEN = 4
Z_ODD = 4
X_EVEN = 6
X_ODD = 6
SUB = B // PARTS
MESH = pl.DeviceIdType.MESH
HI = lax.Precision.HIGHEST
VMEM_LIMIT = 66 * 1000 * 1000

T_INV = 0
T_SEL = 192
T_COL = 384
T_ROW = 640
T_ORD = 832
T_LEN = 834


def routing_table(child_map, child_order):
    kids, tiles = child_map.shape
    tile = jnp.arange(tiles, dtype=jnp.int32)
    place = jnp.arange(96, dtype=jnp.int32)
    hit = child_map[:, None, :] == place[None, :, None]
    inverse = jnp.sum(jnp.where(hit, tile[None, None, :] + 1, 0), axis=2) - 1
    window = child_map // 12
    same = (
        ((tile[:, None] - tile[None, :]) % ROWS == 0)
        & (tile[None, :] < tile[:, None])
    )
    rank = jnp.sum(
        (same[None] & (window[:, :, None] == window[:, None, :])).astype(jnp.int32), axis=2
    )
    slot = tile[None, :] % ROWS + ROWS * rank
    select = jnp.sum(jnp.where(hit, slot[:, None, :], 0), axis=2)
    grouped = child_map.reshape(kids, 8, 8)
    dest = jnp.arange(COLS, dtype=jnp.int32)
    step = jnp.arange(8, dtype=jnp.int32)
    col_pick = jnp.sum(
        jnp.where(
            (grouped // 6)[:, :, :, None] == dest[None, None, None, :],
            step[None, :, None, None],
            0,
        ),
        axis=1,
    )
    edges = jnp.arange(9, dtype=jnp.int32) * 12
    count = jnp.sum((grouped[:, :, :, None] < edges).astype(jnp.int32), axis=1)
    low, mid = count[:, :, 0:8:2], count[:, :, 1:9:2]
    extra = jnp.where(mid - low == 2, low + 1, mid + 1)
    row_pick = jnp.minimum(jnp.stack([low, mid, extra], axis=-1), 7)
    return jnp.concatenate(
        [
            inverse.reshape(-1),
            select.reshape(-1),
            col_pick.reshape(-1),
            row_pick.reshape(-1),
            child_order.reshape(-1),
        ]
    ).astype(jnp.int32)


def enter(row, col):
    barrier = pltpu.get_barrier_semaphore()
    for d in range(1, COLS):
        pl.semaphore_signal(
            barrier,
            inc=1,
            device_id={"col": lax.rem(col + d, COLS)},
            device_id_type=MESH,
        )
    for d in range(1, ROWS):
        pl.semaphore_signal(
            barrier,
            inc=1,
            device_id={"row": lax.rem(row + d, ROWS)},
            device_id_type=MESH,
        )
    pl.semaphore_wait(barrier, COLS + ROWS - 2)


def mul(a, b, ca, cb):
    return lax.dot_general(
        a,
        b,
        (((ca,), (cb,)), ((), ())),
        precision=HI,
        preferred_element_type=jnp.float32,
    )


def eliminate(work, first, last):
    wide = lax.broadcasted_iota(jnp.int32, (B, B), 1)
    one = lax.broadcasted_iota(jnp.int32, (1, B), 1)
    down = lax.broadcasted_iota(jnp.int32, (B, 1), 0)

    def body(j, carry):
        pivot_row = work[pl.ds(j, 1), :]
        pivot = jnp.sum(jnp.where(one == j, pivot_row[:, :B], 0.0), axis=1, keepdims=True)
        column = jnp.sum(jnp.where(wide == j, work[:, :B], 0.0), axis=1, keepdims=True)
        factor = jnp.where(down > j, column * (1.0 / pivot), 0.0)
        work[...] = work[...] - factor * pivot_row
        return carry

    lax.fori_loop(first, last, body, 0)


def eliminated(work):
    wide = lax.broadcasted_iota(jnp.int32, (B, B), 1)
    tall = lax.broadcasted_iota(jnp.int32, (B, B), 0)
    upper = work[:, :B]
    diagonal = jnp.sum(jnp.where(wide == tall, upper, 0.0), axis=1, keepdims=True)
    scale = lax.rsqrt(diagonal)
    scale = scale * (1.5 - 0.5 * diagonal * scale * scale)
    upper_factor = jnp.where(wide >= tall, upper * scale, 0.0)
    inverse = jnp.where(wide <= tall, work[:, B:] * scale, 0.0)
    return upper_factor, inverse


def front_kernel(
    tab,
    parent,
    child,
    out,
    kid_cols,
    send_c,
    send_r,
    send_p,
    recv_p,
    late,
    corner,
    mine,
    rows_ref,
    work,
    lower,
    inv,
    left,
    right,
    load_sem,
    cs,
    cr,
    rs,
    dr,
    br,
    fs,
    ps,
    pr,
    s_a,
    s_u,
    s_p,
    r_p,
    misc,
    *rest,
):
    recv_c = rest[:PARTS]
    recv_r = rest[PARTS:]
    row = lax.axis_index("row")
    col = lax.axis_index("col")
    chip = row // 2
    core = lax.rem(row, 2)
    other = 1 - core
    mate = row + 1 - 2 * core
    kid = col // 8
    slot = lax.rem(col, 8)
    zed = col // 4
    ex = lax.rem(col, 4)
    piece = lax.rem(ex, 2)
    owner = col // 2 == row
    holder = ex // 2 == core
    top = row == 0
    first = top & (col == 0)
    relay = (core == 0) & (row > 0)
    loads = [
        pltpu.make_async_copy(
            child.at[:, k * B : (k + 1) * B], kid_cols.at[k], load_sem.at[k]
        )
        for k in range(8)
    ]
    loads.append(pltpu.make_async_copy(parent, out, load_sem.at[8]))
    for load in loads:
        load.start()
    enter(row, col)
    for load in loads:
        load.wait()

    def copy(src, dst, send, recv, **where):
        return pltpu.make_async_remote_copy(
            src_ref=src,
            dst_ref=dst,
            send_sem=send,
            recv_sem=recv,
            device_id=where,
            device_id_type=MESH,
        )

    def pick_col(dest):
        return tab[T_COL + (kid * 8 + slot) * COLS + dest]

    def take_col(g, dest):
        k = pick_col(dest)
        return [kid_cols[k, t * B + g * SUB : t * B + (g + 1) * SUB, :] for t in range(8)]

    def col_copy(g, d):
        dest = lax.rem(col + d, COLS)
        return copy(
            send_c.at[g, dest], recv_c[g].at[col], cs.at[g, d], cr.at[g, col], col=dest
        )

    def col_arrival(g, d):
        source = lax.rem(col + d, COLS)
        return copy(
            send_c.at[g, source], recv_c[g].at[source], cs.at[g, d], cr.at[g, source], col=source
        )

    def pack_cols(g):
        @pl.loop(1, COLS)
        def _(d):
            dest = lax.rem(col + d, COLS)
            for t, part in enumerate(take_col(g, dest)):
                send_c[g, dest, t] = part

        for t, part in enumerate(take_col(g, col)):
            recv_c[g][col, t] = part

    def send_cols(g):
        @pl.loop(1, COLS)
        def _(d):
            col_copy(g, d).start()

    def panel_copy(d):
        dest = lax.rem(col + d, COLS)
        return copy(send_p.at[dest], recv_p.at[col], ps.at[d], pr.at[col], col=dest)

    def panel_arrival(d):
        source = lax.rem(col + d, COLS)
        return copy(send_p.at[source], recv_p.at[source], ps.at[d], pr.at[source], col=source)

    def late_copy():
        return copy(late, late, misc.at[0], misc.at[1], row=0)

    def late_arrival():
        return copy(late, late, misc.at[0], misc.at[1], row=1)

    def corner_x(d):
        return copy(mine.at[:, 0:NPIV], corner, s_a.at[d - 1], misc.at[2], col=d)

    def corner_z(d):
        return copy(corner, corner, s_a.at[2 + d], misc.at[2], col=4 * d + ex)

    def corner_mate():
        return copy(corner, corner, s_a.at[6], misc.at[2], row=row + 1)

    def corner_arrival():
        return copy(corner, corner, s_a.at[6], misc.at[2], row=row)

    def mine_copy(index, **where):
        return copy(mine, mine, s_u.at[index], misc.at[3], **where)

    def z_copy(d):
        to = lax.rem(zed + d, 4) * 4 + ex
        return copy(mine, rows_ref.at[piece], s_p.at[d - 1], r_p.at[piece], col=to)

    def x_copy(d):
        to = zed * 4 + lax.rem(ex + d, 4)
        return copy(
            rows_ref.at[piece], rows_ref.at[piece], s_p.at[2 + d], r_p.at[piece], col=to
        )

    def piece_arrival(index):
        return copy(mine, rows_ref.at[index], s_p.at[0], r_p.at[index], col=col)

    pack_cols(0)
    send_cols(0)

    @pl.when(row < 2)
    def _():
        @pl.loop(1, COLS)
        def _(d):
            dest = lax.rem(col + d, COLS)
            send_p[dest] = kid_cols[pick_col(dest), 0:B, :]

        recv_p[col] = kid_cols[pick_col(col), 0:B, :]

        @pl.loop(1, COLS)
        def _(d):
            panel_copy(d).start()

    pack_cols(1)
    send_cols(1)
    for g in range(2, PARTS):
        pack_cols(g)

    def direct_copy(g, dy, side):
        chip_to = lax.rem(chip + dy, 4)
        return copy(
            send_r.at[g, chip_to * 3 + side],
            recv_r[g].at[row],
            rs.at[g, dy * 3 + side],
            dr.at[g, row],
            row=chip_to * 2 + side,
        )

    def mate_copy(g):
        return copy(
            send_r.at[g, chip * 3 + other], recv_r[g].at[row], rs.at[g, 0], dr.at[g, row], row=mate
        )

    def extra_copy(g, dy):
        chip_to = lax.rem(chip + dy, 4)
        return copy(
            send_r.at[g, chip_to * 3 + 2],
            recv_r[g].at[8 + row],
            rs.at[g, dy * 3 + 2],
            br.at[g, row],
            row=chip_to * 2 + core,
        )

    def row_arrival(g, source, base, sem):
        return copy(
            send_r.at[g, 0], recv_r[g].at[base + source], rs.at[g, 0], sem.at[g, source], row=source
        )

    def forward_copy(g, dy):
        source = lax.rem(chip + dy, 4) * 2 + core
        return copy(
            recv_r[g].at[8 + source],
            recv_r[g].at[8 + source],
            fs.at[g, dy],
            br.at[g, source],
            row=mate,
        )

    def await_cols(g):
        @pl.loop(1, COLS)
        def _(d):
            col_arrival(g, d).wait_recv()

    def spread_rows(g):
        sources = []
        for h in range(2):
            for b in range(6):
                j = jnp.maximum(tab[T_INV + h * 96 + col * 6 + b], 0)
                sources.append(h * 8 + lax.rem(j, 8))

        @pl.loop(0, 12)
        def _(q):
            for h in range(2):
                k = tab[T_ROW + (h * 8 + row) * 12 + q]
                for b in range(6):
                    send_r[g, q, h, :, b * B : (b + 1) * B] = recv_c[g][sources[h * 6 + b], k]

        recv_r[g][row] = send_r[g, chip * 3 + core]
        recv_r[g][8 + row] = send_r[g, chip * 3 + 2]
        for dy in (2, 1, 3):
            extra_copy(g, dy).start()
            direct_copy(g, dy, 0).start()
            direct_copy(g, dy, 1).start()
        mate_copy(g).start()
        forward_copy(g, 0).start()

    def forward(g):
        for dy in range(1, 4):
            row_arrival(g, lax.rem(chip + dy, 4) * 2 + core, 8, br).wait_recv()
            forward_copy(g, dy).start()

    lane = lax.broadcasted_iota(jnp.int32, (1, B), 1)

    def land(g):
        for d in range(1, ROWS):
            row_arrival(g, lax.rem(row + d, ROWS), 0, dr).wait_recv()
        for dy in range(4):
            row_arrival(g, lax.rem(chip + dy, 4) * 2 + other, 8, br).wait_recv()
        alive = []
        for h in range(2):
            for b in range(6):
                j = tab[T_INV + h * 96 + col * 6 + b]
                limit = jnp.where(j < 0, 0, tab[T_ORD + h] - j * B)
                if b < 2:
                    limit = jnp.where(col == 0, 0, limit)
                alive.append(lane < limit)
        down = lax.broadcasted_iota(jnp.int32, (SUB, 1), 0) + g * SUB

        @pl.loop(0, 12)
        def _(a):
            start = pl.multiple_of(a * B + g * SUB, SUB)
            picks, lives = [], []
            for h in range(2):
                place = h * 96 + row * 12 + a
                i = tab[T_INV + place]
                limit = jnp.where(i < 0, 0, tab[T_ORD + h] - i * B)
                limit = jnp.where(row * 12 + a < 2, 0, limit)
                picks.append(tab[T_SEL + place])
                lives.append(down < limit)
            for b in range(6):
                span = slice(b * B, (b + 1) * B)
                total = out[pl.ds(start, SUB), span]
                for h in range(2):
                    part = recv_r[g][picks[h], h, :, span]
                    total = total + jnp.where(lives[h] & alive[h * 6 + b], part, 0.0)
                out[pl.ds(start, SUB), span] = total

    def frame(place, who, b):
        total = jnp.zeros((B, B), jnp.float32)
        for h in range(2):
            j = tab[T_INV + h * 96 + col * 6 + b]
            source = h * 8 + lax.rem(jnp.maximum(j, 0), 8)
            limit = jnp.where(j < 0, 0, tab[T_ORD + h] - j * B)
            limit = jnp.where(tab[T_INV + h * 96 + place] == who, limit, 0)
            total = total + jnp.where(lane < limit, recv_p[source], 0.0)
        return total

    tall = lax.broadcasted_iota(jnp.int32, (B, B), 0)
    wide = lax.broadcasted_iota(jnp.int32, (B, B), 1)

    def gather_panel():
        @pl.when(row < 2)
        def _():
            @pl.loop(1, COLS)
            def _(d):
                panel_arrival(d).wait_recv()

        @pl.when(row == 1)
        def _():
            for b in range(6):
                late[:, b * B : (b + 1) * B] = frame(1, 1, b)
            late_copy().start()

        @pl.when(top)
        def _():
            for place in range(2):
                here = slice(place * B, (place + 1) * B)
                for b in range(6):
                    span = slice(b * B, (b + 1) * B)
                    mine[here, span] = out[here, span] + frame(place, 0, b)
            late_arrival().wait_recv()
            mine[B:, :] = mine[B:, :] + late[...]

        @pl.when(top)
        def _():
            for d in (2, 6, 1):
                mine_copy(d, row=d).start()

        share_corner_x(top)

    def share_mine():
        for d in (2, 1, 3):
            z_copy(d).start()
        rows_ref[piece] = mine[...]

    def share_corner_x(who):
        @pl.when(who & (col == 0))
        def _():
            for d in (2, 1, 3):
                corner_x(d).start()
            corner[...] = mine[:, 0:NPIV]

    def share_corner_z(who):
        @pl.when(who & (col > 0) & (col < 4))
        def _():
            corner_arrival().wait_recv()

        @pl.when(who & (col < 4))
        def _():
            for d in (2, 1, 3):
                corner_z(d).start()

    def share_corner_mate(who):
        @pl.when(who & (col > 3))
        def _():
            corner_arrival().wait_recv()

        @pl.when(who)
        def _():
            corner_mate().start()

    def half_copy(n):
        half = mine.at[n * B : (n + 1) * B]
        return copy(half, half, s_u.at[3], misc.at[3 + n], row=4)

    def take_mine(who):
        @pl.when(who & (row != 4))
        def _():
            mine_copy(0, row=row).wait_recv()

        @pl.when(who & (row == 2))
        def _():
            half_copy(0).start()

        @pl.when(who & (row == 6))
        def _():
            half_copy(1).start()

        @pl.when(who & (row == 4))
        def _():
            half_copy(0).wait_recv()
            half_copy(1).wait_recv()

        share_corner_x(who & (core == 0))

        @pl.when(who & (core == 0))
        def _():
            mine_copy(4, row=row + 1).start()

    def share_z(who):
        @pl.when(who & owner)
        def _():
            share_mine()

    def share_rows(who):
        @pl.when(who & holder & jnp.logical_not(owner))
        def _():
            piece_arrival(piece).wait_recv()

        @pl.when(who & holder)
        def _():
            for d in (2, 1, 3):
                x_copy(d).start()

    below = row > 1

    def panel_step(g):
        if g == 0:
            gather_panel()
        if g == 1:
            take_mine(row == 1)
        if g == 2:
            share_corner_z(top)
            take_mine(relay & (row != 4))
        if g == 3:
            take_mine(row == 4)
            take_mine(below & (core == 1) & (row != 5))
        if g == 4:
            take_mine(row == 5)
            share_corner_mate(top)
            share_corner_z(relay)
        if g == 5:
            share_corner_mate(relay)
        if g == Z_EVEN:
            share_z(core == 0)
        if g == Z_ODD:
            share_z(core == 1)
        if g == X_EVEN:
            share_rows(core == 0)
        if g == X_ODD:
            share_rows(core == 1)

    def first_block():
        @pl.when(core == 1)
        def _():
            corner_arrival().wait_recv()

        work[:, :B] = corner[:B, :B]
        work[:, B:] = (tall == wide).astype(jnp.float32)
        eliminate(work, 0, B - 1)
        up, low_inv = eliminated(work)
        low21 = mul(corner[B:, :B], low_inv, 1, 1)
        inv[:B, :B] = low_inv
        inv[:B, B:] = jnp.zeros((B, B), jnp.float32)
        lower[:B, :B] = up.T
        lower[:B, B:] = jnp.zeros((B, B), jnp.float32)
        lower[B:, :B] = low21
        work[:, :B] = corner[B:, B:] - mul(low21, low21, 1, 1)
        work[:, B:] = (tall == wide).astype(jnp.float32)

    def second_block():
        eliminate(work, 0, B - 1)
        up, low_inv = eliminated(work)
        inv[B:, B:] = low_inv
        inv[B:, :B] = -mul(low_inv, mul(lower[B:, :B], inv[:B, :B], 1, 0), 1, 0)
        lower[B:, B:] = up.T

    def solve_own():
        right[...] = mul(inv[...], mine[...], 1, 0)

    def solve_rows():
        for index in range(2):

            @pl.when(jnp.logical_not(holder & (piece == index)))
            def _():
                piece_arrival(index).wait_recv()

            left[index] = mul(inv[...], rows_ref[index], 1, 0)

    def update():
        @pl.loop(0, 6)
        def _(n):
            block = left[n // 3, :, pl.ds(pl.multiple_of(lax.rem(n, 3) * NPIV, NPIV), NPIV)]
            here = pl.ds(pl.multiple_of(n * NPIV, NPIV), NPIV)
            out[here, :] = out[here, :] - mul(block, right[...], 0, 0)

            @pl.when(col == 0)
            def _():
                out[here, 0:NPIV] = block.T

        @pl.when(top)
        def _():
            out[0:NPIV, :] = jnp.zeros((NPIV, out.shape[1]), jnp.float32)

        @pl.when(first)
        def _():
            out[0:NPIV, 0:NPIV] = lower[...]

    for g in range(PARTS):
        await_cols(g)
        spread_rows(g)
        panel_step(g)
        if g + 2 < PARTS:
            send_cols(g + 2)
        if g >= 2:
            forward(g - 2)
        if g >= 3:
            land(g - 3)
        if g == 5:
            first_block()
        if g == 6:
            second_block()
        if g == 7:
            solve_own()
    panel_step(PARTS)
    for g in range(PARTS - 2, PARTS - 1):
        forward(g)
    for g in range(PARTS - 3, PARTS - 2):
        land(g)
    solve_rows()
    update()
    land(PARTS - 2)
    forward(PARTS - 1)
    land(PARTS - 1)

    for g in range(PARTS):

        @pl.loop(1, COLS)
        def _(d):
            col_copy(g, d).wait_send()

        for dy in range(1, 4):
            direct_copy(g, dy, 0).wait_send()
            direct_copy(g, dy, 1).wait_send()
            extra_copy(g, dy).wait_send()
        mate_copy(g).wait_send()
        for dy in range(4):
            forward_copy(g, dy).wait_send()

    @pl.when(row < 2)
    def _():
        @pl.loop(1, COLS)
        def _(d):
            panel_copy(d).wait_send()

    @pl.when(row == 1)
    def _():
        late_copy().wait_send()

    @pl.when((core == 0) & (col == 0))
    def _():
        for d in range(1, 4):
            corner_x(d).wait_send()

    @pl.when((core == 0) & (col < 4))
    def _():
        for d in range(1, 4):
            corner_z(d).wait_send()

    @pl.when(core == 0)
    def _():
        corner_mate().wait_send()

    @pl.when(top)
    def _():
        for d in (2, 6, 1):
            mine_copy(d, row=d).wait_send()

    @pl.when(relay)
    def _():
        mine_copy(4, row=row + 1).wait_send()

    @pl.when(row == 2)
    def _():
        half_copy(0).wait_send()

    @pl.when(row == 6)
    def _():
        half_copy(1).wait_send()

    @pl.when(owner)
    def _():
        for d in (2, 1, 3):
            z_copy(d).wait_send()

    @pl.when(holder)
    def _():
        for d in (2, 1, 3):
            x_copy(d).wait_send()


def shards(parent_front, child_blocks, child_map, child_order):
    table = routing_table(child_map, child_order)
    width = parent_front.shape[1]
    wild = pl.BlockSpec(memory_space=pl.ANY)

    def vmem(*shape):
        return pltpu.VMEM(shape, jnp.float32)

    dma = pltpu.SemaphoreType.DMA
    return pl.pallas_call(
        front_kernel,
        out_shape=jax.ShapeDtypeStruct(parent_front.shape, jnp.float32),
        in_specs=[pl.BlockSpec(memory_space=pltpu.SMEM), wild, wild],
        out_specs=pl.BlockSpec(memory_space=pltpu.VMEM),
        scratch_shapes=[
            vmem(8, 8 * B, B),
            vmem(PARTS, COLS, 8, SUB, B),
            vmem(PARTS, 12, 2, SUB, width),
            vmem(COLS, B, B),
            vmem(COLS, B, B),
            vmem(B, width),
            vmem(NPIV, NPIV),
            vmem(NPIV, width),
            vmem(2, NPIV, width),
            vmem(B, 2 * B),
            vmem(NPIV, NPIV),
            vmem(NPIV, NPIV),
            vmem(2, NPIV, width),
            vmem(NPIV, width),
            dma((9,)),
            dma((PARTS, COLS)),
            dma((PARTS, COLS)),
            dma((PARTS, 12)),
            dma((PARTS, ROWS)),
            dma((PARTS, ROWS)),
            dma((PARTS, 4)),
            dma((COLS,)),
            dma((COLS,)),
            dma((7,)),
            dma((8,)),
            dma((6,)),
            dma((2,)),
            dma((5,)),
        ]
        + [vmem(COLS, 8, SUB, B)] * PARTS
        + [vmem(16, 2, SUB, width)] * PARTS,
        compiler_params=pltpu.CompilerParams(
            collective_id=0, has_side_effects=True, vmem_limit_bytes=VMEM_LIMIT
        ),
        name="front",
    )(table, parent_front, child_blocks)


def solution(mesh):
    placed = (P("row", "col"), P("row", "col"), P(), P())
    return jax.shard_map(
        shards, mesh=mesh, in_specs=placed, out_specs=P("row", "col"), check_vma=False
    )
```

```python
import functools

import jax
import jax.numpy as jnp
from jax import lax
from jax.experimental import pallas as pl
from jax.experimental.pallas import tpu as pltpu
from jax.sharding import PartitionSpec as P

B = 128
NPIV = 256
ROWS = 8
COLS = 16
PARTS = 8
Z_EVEN = 4
Z_ODD = 4
X_EVEN = 6
X_ODD = 6
SUB = B // PARTS
MESH = pl.DeviceIdType.MESH
HI = lax.Precision.HIGHEST
VMEM_LIMIT = 56 * 1000 * 1000

T_INV = 0
T_SEL = 192
T_COL = 384
T_ROW = 640
T_ORD = 832
T_LEN = 834


def routing_table(child_map, child_order):
    kids, tiles = child_map.shape
    tile = jnp.arange(tiles, dtype=jnp.int32)
    place = jnp.arange(96, dtype=jnp.int32)
    hit = child_map[:, None, :] == place[None, :, None]
    inverse = jnp.sum(jnp.where(hit, tile[None, None, :] + 1, 0), axis=2) - 1
    window = child_map // 12
    same = (
        ((tile[:, None] - tile[None, :]) % ROWS == 0)
        & (tile[None, :] < tile[:, None])
    )
    rank = jnp.sum(
        (same[None] & (window[:, :, None] == window[:, None, :])).astype(jnp.int32), axis=2
    )
    slot = tile[None, :] % ROWS + ROWS * rank
    select = jnp.sum(jnp.where(hit, slot[:, None, :], 0), axis=2)
    grouped = child_map.reshape(kids, 8, 8)
    dest = jnp.arange(COLS, dtype=jnp.int32)
    step = jnp.arange(8, dtype=jnp.int32)
    col_pick = jnp.sum(
        jnp.where(
            (grouped // 6)[:, :, :, None] == dest[None, None, None, :],
            step[None, :, None, None],
            0,
        ),
        axis=1,
    )
    edges = jnp.arange(9, dtype=jnp.int32) * 12
    count = jnp.sum((grouped[:, :, :, None] < edges).astype(jnp.int32), axis=1)
    low, mid = count[:, :, 0:8:2], count[:, :, 1:9:2]
    extra = jnp.where(mid - low == 2, low + 1, mid + 1)
    row_pick = jnp.minimum(jnp.stack([low, mid, extra], axis=-1), 7)
    return jnp.concatenate(
        [
            inverse.reshape(-1),
            select.reshape(-1),
            col_pick.reshape(-1),
            row_pick.reshape(-1),
            child_order.reshape(-1),
        ]
    ).astype(jnp.int32)


def enter(row, col):
    barrier = pltpu.get_barrier_semaphore()
    for d in range(1, COLS):
        pl.semaphore_signal(
            barrier,
            inc=1,
            device_id={"col": lax.rem(col + d, COLS)},
            device_id_type=MESH,
        )
    for d in range(1, ROWS):
        pl.semaphore_signal(
            barrier,
            inc=1,
            device_id={"row": lax.rem(row + d, ROWS)},
            device_id_type=MESH,
        )
    pl.semaphore_wait(barrier, COLS + ROWS - 2)


def mul(a, b, ca, cb):
    return lax.dot_general(
        a,
        b,
        (((ca,), (cb,)), ((), ())),
        precision=HI,
        preferred_element_type=jnp.float32,
    )


def eliminate(work, first, last):
    wide = lax.broadcasted_iota(jnp.int32, (B, B), 1)
    one = lax.broadcasted_iota(jnp.int32, (1, B), 1)
    down = lax.broadcasted_iota(jnp.int32, (B, 1), 0)

    def body(j, carry):
        pivot_row = work[pl.ds(j, 1), :]
        pivot = jnp.sum(jnp.where(one == j, pivot_row[:, :B], 0.0), axis=1, keepdims=True)
        column = jnp.sum(jnp.where(wide == j, work[:, :B], 0.0), axis=1, keepdims=True)
        factor = jnp.where(down > j, column * (1.0 / pivot), 0.0)
        work[...] = work[...] - factor * pivot_row
        return carry

    lax.fori_loop(first, last, body, 0)


def eliminated(work):
    wide = lax.broadcasted_iota(jnp.int32, (B, B), 1)
    tall = lax.broadcasted_iota(jnp.int32, (B, B), 0)
    upper = work[:, :B]
    diagonal = jnp.sum(jnp.where(wide == tall, upper, 0.0), axis=1, keepdims=True)
    scale = lax.rsqrt(diagonal)
    scale = scale * (1.5 - 0.5 * diagonal * scale * scale)
    upper_factor = jnp.where(wide >= tall, upper * scale, 0.0)
    inverse = jnp.where(wide <= tall, work[:, B:] * scale, 0.0)
    return upper_factor, inverse


def front_kernel(
    tab,
    parent,
    child,
    out,
    kid_cols,
    send_c,
    send_r,
    send_p,
    recv_p,
    late,
    corner,
    mine,
    rows_ref,
    work,
    lower,
    inv,
    left,
    right,
    load_sem,
    cs,
    cr,
    rs,
    dr,
    br,
    fs,
    ps,
    pr,
    s_a,
    s_u,
    s_p,
    r_p,
    misc,
    *rest,
):
    recv_c = rest[:PARTS]
    recv_r = rest[PARTS:]
    row = lax.axis_index("row")
    col = lax.axis_index("col")
    chip = row // 2
    core = lax.rem(row, 2)
    other = 1 - core
    mate = row + 1 - 2 * core
    kid = col // 8
    slot = lax.rem(col, 8)
    zed = col // 4
    ex = lax.rem(col, 4)
    piece = lax.rem(ex, 2)
    owner = col // 2 == row
    holder = ex // 2 == core
    top = row == 0
    first = top & (col == 0)
    relay = (core == 0) & (row > 0)
    loads = [
        pltpu.make_async_copy(
            child.at[:, k * B : (k + 1) * B], kid_cols.at[k], load_sem.at[k]
        )
        for k in range(8)
    ]
    loads.append(pltpu.make_async_copy(parent, out, load_sem.at[8]))
    for load in loads:
        load.start()
    enter(row, col)
    for load in loads:
        load.wait()

    def copy(src, dst, send, recv, **where):
        return pltpu.make_async_remote_copy(
            src_ref=src,
            dst_ref=dst,
            send_sem=send,
            recv_sem=recv,
            device_id=where,
            device_id_type=MESH,
        )

    def pick_col(dest):
        return tab[T_COL + (kid * 8 + slot) * COLS + dest]

    def take_col(g, dest):
        k = pick_col(dest)
        return [kid_cols[k, t * B + g * SUB : t * B + (g + 1) * SUB, :] for t in range(8)]

    def col_copy(g, d, start):
        dest = lax.rem(col + d, COLS)
        return copy(
            send_c.at[g, dest, start:8],
            recv_c[g].at[col, start:8],
            cs.at[g, d],
            cr.at[g, col],
            col=dest,
        )

    def col_arrival(g, d, start):
        source = lax.rem(col + d, COLS)
        return copy(
            send_c.at[g, source, start:8],
            recv_c[g].at[source, start:8],
            cs.at[g, d],
            cr.at[g, source],
            col=source,
        )

    def each_col(g, action):
        def run(start):
            @pl.loop(1, COLS)
            def _(d):
                action(d, start)

        if g == 0:
            run(0)
        else:

            @pl.when(row < 2)
            def _():
                run(1)

            @pl.when(row > 1)
            def _():
                run(0)

    def pack_cols(g):
        @pl.loop(1, COLS)
        def _(d):
            dest = lax.rem(col + d, COLS)
            for t, part in enumerate(take_col(g, dest)):
                send_c[g, dest, t] = part

        for t, part in enumerate(take_col(g, col)):
            recv_c[g][col, t] = part

    def send_cols(g):
        each_col(g, lambda d, start: col_copy(g, d, start).start())

    def panel_copy(d):
        dest = lax.rem(col + d, COLS)
        return copy(send_p.at[dest], recv_p.at[col], ps.at[d], pr.at[col], col=dest)

    def panel_arrival(d):
        source = lax.rem(col + d, COLS)
        return copy(send_p.at[source], recv_p.at[source], ps.at[d], pr.at[source], col=source)

    def late_copy():
        return copy(late, late, misc.at[0], misc.at[1], row=0)

    def late_arrival():
        return copy(late, late, misc.at[0], misc.at[1], row=1)

    def corner_x(d):
        return copy(mine.at[:, 0:NPIV], corner, s_a.at[d - 1], misc.at[2], col=d)

    def corner_z(d):
        return copy(corner, corner, s_a.at[2 + d], misc.at[2], col=4 * d + ex)

    def corner_mate():
        return copy(corner, corner, s_a.at[6], misc.at[2], row=row + 1)

    def corner_arrival():
        return copy(corner, corner, s_a.at[6], misc.at[2], row=row)

    def mine_copy(index, **where):
        return copy(mine, mine, s_u.at[index], misc.at[3], **where)

    def z_copy(d):
        to = lax.rem(zed + d, 4) * 4 + ex
        return copy(mine, rows_ref.at[piece], s_p.at[d - 1], r_p.at[piece], col=to)

    def x_copy(d):
        to = zed * 4 + lax.rem(ex + d, 4)
        return copy(
            rows_ref.at[piece], rows_ref.at[piece], s_p.at[2 + d], r_p.at[piece], col=to
        )

    def piece_arrival(index):
        return copy(mine, rows_ref.at[index], s_p.at[0], r_p.at[index], col=col)

    pack_cols(0)
    send_cols(0)

    @pl.when(row < 2)
    def _():
        @pl.loop(1, COLS)
        def _(d):
            dest = lax.rem(col + d, COLS)
            send_p[dest] = kid_cols[pick_col(dest), 0:B, :]

        recv_p[col] = kid_cols[pick_col(col), 0:B, :]

        @pl.loop(1, COLS)
        def _(d):
            panel_copy(d).start()

    pack_cols(1)
    send_cols(1)
    for g in range(2, PARTS):
        pack_cols(g)

    def direct_copy(g, dy, side):
        chip_to = lax.rem(chip + dy, 4)
        return copy(
            send_r.at[g, chip_to * 3 + side],
            recv_r[g].at[row],
            rs.at[g, dy * 3 + side],
            dr.at[g, row],
            row=chip_to * 2 + side,
        )

    def mate_copy(g):
        return copy(
            send_r.at[g, chip * 3 + other], recv_r[g].at[row], rs.at[g, 0], dr.at[g, row], row=mate
        )

    def extra_copy(g, dy):
        chip_to = lax.rem(chip + dy, 4)
        return copy(
            send_r.at[g, chip_to * 3 + 2],
            recv_r[g].at[8 + row],
            rs.at[g, dy * 3 + 2],
            br.at[g, row],
            row=chip_to * 2 + core,
        )

    def row_arrival(g, source, base, sem):
        return copy(
            send_r.at[g, 0], recv_r[g].at[base + source], rs.at[g, 0], sem.at[g, source], row=source
        )

    def forward_copy(g, dy):
        source = lax.rem(chip + dy, 4) * 2 + core
        return copy(
            recv_r[g].at[8 + source],
            recv_r[g].at[8 + source],
            fs.at[g, dy],
            br.at[g, source],
            row=mate,
        )

    def await_cols(g):
        each_col(g, lambda d, start: col_arrival(g, d, start).wait_recv())

    def spread_rows(g):
        sources = []
        for h in range(2):
            for b in range(6):
                j = jnp.maximum(tab[T_INV + h * 96 + col * 6 + b], 0)
                sources.append(h * 8 + lax.rem(j, 8))

        @pl.loop(0, 12)
        def _(q):
            for h in range(2):
                k = tab[T_ROW + (h * 8 + row) * 12 + q]
                for b in range(6):
                    send_r[g, q, h, :, b * B : (b + 1) * B] = recv_c[g][sources[h * 6 + b], k]

        recv_r[g][row] = send_r[g, chip * 3 + core]
        recv_r[g][8 + row] = send_r[g, chip * 3 + 2]
        for dy in (2, 1, 3):
            extra_copy(g, dy).start()
            direct_copy(g, dy, 0).start()
            direct_copy(g, dy, 1).start()
        mate_copy(g).start()
        forward_copy(g, 0).start()

    def forward(g):
        for dy in range(1, 4):
            row_arrival(g, lax.rem(chip + dy, 4) * 2 + core, 8, br).wait_recv()
            forward_copy(g, dy).start()

    lane = lax.broadcasted_iota(jnp.int32, (1, B), 1)

    def land(g):
        for d in range(1, ROWS):
            row_arrival(g, lax.rem(row + d, ROWS), 0, dr).wait_recv()
        for dy in range(4):
            row_arrival(g, lax.rem(chip + dy, 4) * 2 + other, 8, br).wait_recv()
        alive = []
        for h in range(2):
            for b in range(6):
                j = tab[T_INV + h * 96 + col * 6 + b]
                limit = jnp.where(j < 0, 0, tab[T_ORD + h] - j * B)
                if b < 2:
                    limit = jnp.where(col == 0, 0, limit)
                alive.append(lane < limit)
        down = lax.broadcasted_iota(jnp.int32, (SUB, 1), 0) + g * SUB

        @pl.loop(0, 12)
        def _(a):
            start = pl.multiple_of(a * B + g * SUB, SUB)
            picks, lives = [], []
            for h in range(2):
                place = h * 96 + row * 12 + a
                i = tab[T_INV + place]
                limit = jnp.where(i < 0, 0, tab[T_ORD + h] - i * B)
                limit = jnp.where(row * 12 + a < 2, 0, limit)
                picks.append(tab[T_SEL + place])
                lives.append(down < limit)
            for b in range(6):
                span = slice(b * B, (b + 1) * B)
                total = out[pl.ds(start, SUB), span]
                for h in range(2):
                    part = recv_r[g][picks[h], h, :, span]
                    total = total + jnp.where(lives[h] & alive[h * 6 + b], part, 0.0)
                out[pl.ds(start, SUB), span] = total

    def frame(place, who, b):
        total = jnp.zeros((B, B), jnp.float32)
        for h in range(2):
            j = tab[T_INV + h * 96 + col * 6 + b]
            source = h * 8 + lax.rem(jnp.maximum(j, 0), 8)
            limit = jnp.where(j < 0, 0, tab[T_ORD + h] - j * B)
            limit = jnp.where(tab[T_INV + h * 96 + place] == who, limit, 0)
            total = total + jnp.where(lane < limit, recv_p[source], 0.0)
        return total

    tall = lax.broadcasted_iota(jnp.int32, (B, B), 0)
    wide = lax.broadcasted_iota(jnp.int32, (B, B), 1)

    def gather_panel():
        @pl.when(row < 2)
        def _():
            @pl.loop(1, COLS)
            def _(d):
                panel_arrival(d).wait_recv()

            @pl.loop(0, COLS)
            def _(source):
                for g in range(1, PARTS):
                    recv_c[g][source, 0] = recv_p[source, g * SUB : (g + 1) * SUB, :]

        @pl.when(row == 1)
        def _():
            for b in range(6):
                late[:, b * B : (b + 1) * B] = frame(1, 1, b)
            late_copy().start()

        @pl.when(top)
        def _():
            for place in range(2):
                here = slice(place * B, (place + 1) * B)
                for b in range(6):
                    span = slice(b * B, (b + 1) * B)
                    mine[here, span] = out[here, span] + frame(place, 0, b)
            late_arrival().wait_recv()
            mine[B:, :] = mine[B:, :] + late[...]

        @pl.when(top)
        def _():
            for d in (2, 6, 1):
                mine_copy(d, row=d).start()

        share_corner_x(top)

    def share_mine():
        for d in (2, 1, 3):
            z_copy(d).start()
        rows_ref[piece] = mine[...]

    def share_corner_x(who):
        @pl.when(who & (col == 0))
        def _():
            for d in (2, 1, 3):
                corner_x(d).start()
            corner[...] = mine[:, 0:NPIV]

    def share_corner_z(who):
        @pl.when(who & (col > 0) & (col < 4))
        def _():
            corner_arrival().wait_recv()

        @pl.when(who & (col < 4))
        def _():
            for d in (2, 1, 3):
                corner_z(d).start()

    def share_corner_mate(who):
        @pl.when(who & (col > 3))
        def _():
            corner_arrival().wait_recv()

        @pl.when(who)
        def _():
            corner_mate().start()

    def half_copy(n):
        half = mine.at[n * B : (n + 1) * B]
        return copy(half, half, s_u.at[3], misc.at[3 + n], row=4)

    def take_mine(who):
        @pl.when(who & (row != 4))
        def _():
            mine_copy(0, row=row).wait_recv()

        @pl.when(who & (row == 2))
        def _():
            half_copy(0).start()

        @pl.when(who & (row == 6))
        def _():
            half_copy(1).start()

        @pl.when(who & (row == 4))
        def _():
            half_copy(0).wait_recv()
            half_copy(1).wait_recv()

        share_corner_x(who & (core == 0))

        @pl.when(who & (core == 0))
        def _():
            mine_copy(4, row=row + 1).start()

    def share_z(who):
        @pl.when(who & owner)
        def _():
            share_mine()

    def share_rows(who):
        @pl.when(who & holder & jnp.logical_not(owner))
        def _():
            piece_arrival(piece).wait_recv()

        @pl.when(who & holder)
        def _():
            for d in (2, 1, 3):
                x_copy(d).start()

    below = row > 1

    def panel_step(g):
        if g == 0:
            gather_panel()
        if g == 1:
            take_mine(row == 1)
        if g == 2:
            share_corner_z(top)
            take_mine(relay & (row != 4))
        if g == 3:
            take_mine(row == 4)
            take_mine(below & (core == 1) & (row != 5))
        if g == 4:
            take_mine(row == 5)
            share_corner_mate(top)
            share_corner_z(relay)
        if g == 5:
            share_corner_mate(relay)
        if g == Z_EVEN:
            share_z(core == 0)
        if g == Z_ODD:
            share_z(core == 1)
        if g == X_EVEN:
            share_rows(core == 0)
        if g == X_ODD:
            share_rows(core == 1)

    def first_block():
        @pl.when(core == 1)
        def _():
            corner_arrival().wait_recv()

        work[:, :B] = corner[:B, :B]
        work[:, B:] = (tall == wide).astype(jnp.float32)
        eliminate(work, 0, B - 1)
        up, low_inv = eliminated(work)
        low21 = mul(corner[B:, :B], low_inv, 1, 1)
        inv[:B, :B] = low_inv
        inv[:B, B:] = jnp.zeros((B, B), jnp.float32)
        lower[:B, :B] = up.T
        lower[:B, B:] = jnp.zeros((B, B), jnp.float32)
        lower[B:, :B] = low21
        work[:, :B] = corner[B:, B:] - mul(low21, low21, 1, 1)
        work[:, B:] = (tall == wide).astype(jnp.float32)

    def second_block():
        eliminate(work, 0, B - 1)
        up, low_inv = eliminated(work)
        inv[B:, B:] = low_inv
        inv[B:, :B] = -mul(low_inv, mul(lower[B:, :B], inv[:B, :B], 1, 0), 1, 0)
        lower[B:, B:] = up.T

    def solve_own():
        right[...] = mul(inv[...], mine[...], 1, 0)

    def solve_rows():
        for index in range(2):

            @pl.when(jnp.logical_not(holder & (piece == index)))
            def _():
                piece_arrival(index).wait_recv()

            left[index] = mul(inv[...], rows_ref[index], 1, 0)

    def update():
        @pl.loop(0, 6)
        def _(n):
            block = left[n // 3, :, pl.ds(pl.multiple_of(lax.rem(n, 3) * NPIV, NPIV), NPIV)]
            here = pl.ds(pl.multiple_of(n * NPIV, NPIV), NPIV)
            out[here, :] = out[here, :] - mul(block, right[...], 0, 0)

            @pl.when(col == 0)
            def _():
                out[here, 0:NPIV] = block.T

        @pl.when(top)
        def _():
            out[0:NPIV, :] = jnp.zeros((NPIV, out.shape[1]), jnp.float32)

        @pl.when(first)
        def _():
            out[0:NPIV, 0:NPIV] = lower[...]

    for g in range(PARTS):
        await_cols(g)
        spread_rows(g)
        if g + 2 < PARTS:
            send_cols(g + 2)
        panel_step(g)
        if g >= 2:
            forward(g - 2)
        if g >= 3:
            land(g - 3)
        if g == 5:
            first_block()
        if g == 6:
            second_block()
        if g == 7:
            solve_own()
    panel_step(PARTS)
    for g in range(PARTS - 2, PARTS - 1):
        forward(g)
    for g in range(PARTS - 3, PARTS - 2):
        land(g)
    solve_rows()
    update()
    land(PARTS - 2)
    forward(PARTS - 1)
    land(PARTS - 1)

    for g in range(PARTS):

        each_col(g, lambda d, start: col_copy(g, d, start).wait_send())

        for dy in range(1, 4):
            direct_copy(g, dy, 0).wait_send()
            direct_copy(g, dy, 1).wait_send()
            extra_copy(g, dy).wait_send()
        mate_copy(g).wait_send()
        for dy in range(4):
            forward_copy(g, dy).wait_send()

    @pl.when(row < 2)
    def _():
        @pl.loop(1, COLS)
        def _(d):
            panel_copy(d).wait_send()

    @pl.when(row == 1)
    def _():
        late_copy().wait_send()

    @pl.when((core == 0) & (col == 0))
    def _():
        for d in range(1, 4):
            corner_x(d).wait_send()

    @pl.when((core == 0) & (col < 4))
    def _():
        for d in range(1, 4):
            corner_z(d).wait_send()

    @pl.when(core == 0)
    def _():
        corner_mate().wait_send()

    @pl.when(top)
    def _():
        for d in (2, 6, 1):
            mine_copy(d, row=d).wait_send()

    @pl.when(relay)
    def _():
        mine_copy(4, row=row + 1).wait_send()

    @pl.when(row == 2)
    def _():
        half_copy(0).wait_send()

    @pl.when(row == 6)
    def _():
        half_copy(1).wait_send()

    @pl.when(owner)
    def _():
        for d in (2, 1, 3):
            z_copy(d).wait_send()

    @pl.when(holder)
    def _():
        for d in (2, 1, 3):
            x_copy(d).wait_send()


def shards(parent_front, child_blocks, child_map, child_order):
    table = routing_table(child_map, child_order)
    width = parent_front.shape[1]
    wild = pl.BlockSpec(memory_space=pl.ANY)

    def vmem(*shape):
        return pltpu.VMEM(shape, jnp.float32)

    dma = pltpu.SemaphoreType.DMA
    return pl.pallas_call(
        front_kernel,
        out_shape=pltpu.VMEM(parent_front.shape, jnp.float32),
        in_specs=[pl.BlockSpec(memory_space=pltpu.SMEM), wild, wild],
        out_specs=pl.BlockSpec(memory_space=pltpu.VMEM),
        scratch_shapes=[
            vmem(8, 8 * B, B),
            vmem(PARTS, COLS, 8, SUB, B),
            vmem(PARTS, 12, 2, SUB, width),
            vmem(COLS, B, B),
            vmem(COLS, B, B),
            vmem(B, width),
            vmem(NPIV, NPIV),
            vmem(NPIV, width),
            vmem(2, NPIV, width),
            vmem(B, 2 * B),
            vmem(NPIV, NPIV),
            vmem(NPIV, NPIV),
            vmem(2, NPIV, width),
            vmem(NPIV, width),
            dma((9,)),
            dma((PARTS, COLS)),
            dma((PARTS, COLS)),
            dma((PARTS, 12)),
            dma((PARTS, ROWS)),
            dma((PARTS, ROWS)),
            dma((PARTS, 4)),
            dma((COLS,)),
            dma((COLS,)),
            dma((7,)),
            dma((8,)),
            dma((6,)),
            dma((2,)),
            dma((5,)),
        ]
        + [vmem(COLS, 8, SUB, B)] * PARTS
        + [vmem(16, 2, SUB, width)] * PARTS,
        compiler_params=pltpu.CompilerParams(
            collective_id=0, has_side_effects=True, vmem_limit_bytes=VMEM_LIMIT
        ),
        name="front",
    )(table, parent_front, child_blocks)


def solution(mesh):
    placed = (P("row", "col"), P("row", "col"), P(), P())
    return jax.shard_map(
        shards, mesh=mesh, in_specs=placed, out_specs=P("row", "col"), check_vma=False
    )
```

```python
import functools

import jax
import jax.numpy as jnp
from jax import lax
from jax.experimental import pallas as pl
from jax.experimental.pallas import tpu as pltpu
from jax.sharding import PartitionSpec as P

B = 128
NPIV = 256
ROWS = 8
COLS = 16
PARTS = 8
Z_EVEN = 4
Z_ODD = 4
X_EVEN = 6
X_ODD = 6
SUB = B // PARTS
MESH = pl.DeviceIdType.MESH
HI = lax.Precision.HIGHEST
VMEM_LIMIT = 56 * 1000 * 1000

T_INV = 0
T_SEL = 192
T_COL = 384
T_ROW = 640
T_ORD = 832
T_LEN = 834


def routing_table(child_map, child_order):
    kids, tiles = child_map.shape
    tile = jnp.arange(tiles, dtype=jnp.int32)
    place = jnp.arange(96, dtype=jnp.int32)
    hit = child_map[:, None, :] == place[None, :, None]
    inverse = jnp.sum(jnp.where(hit, tile[None, None, :] + 1, 0), axis=2) - 1
    window = child_map // 12
    same = (
        ((tile[:, None] - tile[None, :]) % ROWS == 0)
        & (tile[None, :] < tile[:, None])
    )
    rank = jnp.sum(
        (same[None] & (window[:, :, None] == window[:, None, :])).astype(jnp.int32), axis=2
    )
    slot = tile[None, :] % ROWS + ROWS * rank
    select = jnp.sum(jnp.where(hit, slot[:, None, :], 0), axis=2)
    grouped = child_map.reshape(kids, 8, 8)
    dest = jnp.arange(COLS, dtype=jnp.int32)
    step = jnp.arange(8, dtype=jnp.int32)
    col_pick = jnp.sum(
        jnp.where(
            (grouped // 6)[:, :, :, None] == dest[None, None, None, :],
            step[None, :, None, None],
            0,
        ),
        axis=1,
    )
    edges = jnp.arange(9, dtype=jnp.int32) * 12
    count = jnp.sum((grouped[:, :, :, None] < edges).astype(jnp.int32), axis=1)
    low, mid = count[:, :, 0:8:2], count[:, :, 1:9:2]
    extra = jnp.where(mid - low == 2, low + 1, mid + 1)
    row_pick = jnp.minimum(jnp.stack([low, mid, extra], axis=-1), 7)
    return jnp.concatenate(
        [
            inverse.reshape(-1),
            select.reshape(-1),
            col_pick.reshape(-1),
            row_pick.reshape(-1),
            child_order.reshape(-1),
        ]
    ).astype(jnp.int32)


def enter(row, col):
    barrier = pltpu.get_barrier_semaphore()
    for d in range(1, COLS):
        pl.semaphore_signal(
            barrier,
            inc=1,
            device_id={"col": lax.rem(col + d, COLS)},
            device_id_type=MESH,
        )
    for d in range(1, ROWS):
        pl.semaphore_signal(
            barrier,
            inc=1,
            device_id={"row": lax.rem(row + d, ROWS)},
            device_id_type=MESH,
        )
    pl.semaphore_wait(barrier, COLS + ROWS - 2)


def mul(a, b, ca, cb):
    return lax.dot_general(
        a,
        b,
        (((ca,), (cb,)), ((), ())),
        precision=HI,
        preferred_element_type=jnp.float32,
    )


def eliminate(work, first, last):
    wide = lax.broadcasted_iota(jnp.int32, (B, B), 1)
    one = lax.broadcasted_iota(jnp.int32, (1, B), 1)
    down = lax.broadcasted_iota(jnp.int32, (B, 1), 0)

    def body(j, carry):
        pivot_row = work[pl.ds(j, 1), :]
        pivot = jnp.sum(jnp.where(one == j, pivot_row[:, :B], 0.0), axis=1, keepdims=True)
        column = jnp.sum(jnp.where(wide == j, work[:, :B], 0.0), axis=1, keepdims=True)
        factor = jnp.where(down > j, column * (1.0 / pivot), 0.0)
        work[...] = work[...] - factor * pivot_row
        return carry

    lax.fori_loop(first, last, body, 0)


def eliminated(work):
    wide = lax.broadcasted_iota(jnp.int32, (B, B), 1)
    tall = lax.broadcasted_iota(jnp.int32, (B, B), 0)
    upper = work[:, :B]
    diagonal = jnp.sum(jnp.where(wide == tall, upper, 0.0), axis=1, keepdims=True)
    scale = lax.rsqrt(diagonal)
    scale = scale * (1.5 - 0.5 * diagonal * scale * scale)
    upper_factor = jnp.where(wide >= tall, upper * scale, 0.0)
    inverse = jnp.where(wide <= tall, work[:, B:] * scale, 0.0)
    return upper_factor, inverse


def front_kernel(
    tab,
    parent,
    child,
    out,
    kid_cols,
    send_c,
    send_r,
    send_p,
    recv_p,
    late,
    corner,
    mine,
    rows_ref,
    work,
    lower,
    inv,
    left,
    right,
    load_sem,
    cs,
    cr,
    rs,
    dr,
    br,
    fs,
    ps,
    pr,
    s_a,
    s_u,
    s_p,
    r_p,
    misc,
    *rest,
):
    recv_c = rest[:PARTS]
    recv_r = rest[PARTS:]
    row = lax.axis_index("row")
    col = lax.axis_index("col")
    chip = row // 2
    core = lax.rem(row, 2)
    other = 1 - core
    mate = row + 1 - 2 * core
    kid = col // 8
    slot = lax.rem(col, 8)
    zed = col // 4
    ex = lax.rem(col, 4)
    piece = lax.rem(ex, 2)
    owner = col // 2 == row
    holder = ex // 2 == core
    top = row == 0
    first = top & (col == 0)
    relay = (core == 0) & (row > 0)
    loads = [
        pltpu.make_async_copy(
            child.at[:, k * B : (k + 1) * B], kid_cols.at[k], load_sem.at[k]
        )
        for k in range(8)
    ]
    loads.append(pltpu.make_async_copy(parent, out, load_sem.at[8]))
    for load in loads:
        load.start()
    enter(row, col)
    for load in loads:
        load.wait()

    def copy(src, dst, send, recv, **where):
        return pltpu.make_async_remote_copy(
            src_ref=src,
            dst_ref=dst,
            send_sem=send,
            recv_sem=recv,
            device_id=where,
            device_id_type=MESH,
        )

    def pick_col(dest):
        return tab[T_COL + (kid * 8 + slot) * COLS + dest]

    def take_col(g, dest):
        k = pick_col(dest)
        return [kid_cols[k, t * B + g * SUB : t * B + (g + 1) * SUB, :] for t in range(8)]

    def col_copy(g, d, start):
        dest = lax.rem(col + d, COLS)
        return copy(
            send_c.at[g, dest, start:8],
            recv_c[g].at[col, start:8],
            cs.at[g, d],
            cr.at[g, col],
            col=dest,
        )

    def col_arrival(g, d, start):
        source = lax.rem(col + d, COLS)
        return copy(
            send_c.at[g, source, start:8],
            recv_c[g].at[source, start:8],
            cs.at[g, d],
            cr.at[g, source],
            col=source,
        )

    def each_col(g, action):
        def run(start):
            @pl.loop(1, COLS)
            def _(d):
                action(d, start)

        if g == 0:
            run(0)
        else:

            @pl.when(row < 2)
            def _():
                run(1)

            @pl.when(row > 1)
            def _():
                run(0)

    def pack_cols(g):
        @pl.loop(1, COLS)
        def _(d):
            dest = lax.rem(col + d, COLS)
            for t, part in enumerate(take_col(g, dest)):
                send_c[g, dest, t] = part

        for t, part in enumerate(take_col(g, col)):
            recv_c[g][col, t] = part

    def send_cols(g):
        each_col(g, lambda d, start: col_copy(g, d, start).start())

    def panel_copy(d):
        dest = lax.rem(col + d, COLS)
        return copy(send_p.at[dest], recv_p.at[col], ps.at[d], pr.at[col], col=dest)

    def panel_arrival(d):
        source = lax.rem(col + d, COLS)
        return copy(send_p.at[source], recv_p.at[source], ps.at[d], pr.at[source], col=source)

    def late_copy():
        return copy(late, late, misc.at[0], misc.at[1], row=0)

    def late_arrival():
        return copy(late, late, misc.at[0], misc.at[1], row=1)

    def corner_x(d):
        return copy(mine.at[:, 0:NPIV], corner, s_a.at[d - 1], misc.at[2], col=d)

    def corner_z(d):
        return copy(corner, corner, s_a.at[2 + d], misc.at[2], col=4 * d + ex)

    def corner_mate():
        return copy(corner, corner, s_a.at[6], misc.at[2], row=row + 1)

    def corner_arrival():
        return copy(corner, corner, s_a.at[6], misc.at[2], row=row)

    def mine_copy(index, **where):
        return copy(mine, mine, s_u.at[index], misc.at[3], **where)

    def z_copy(d):
        to = lax.rem(zed + d, 4) * 4 + ex
        return copy(mine, rows_ref.at[piece], s_p.at[d - 1], r_p.at[piece], col=to)

    def x_copy(d):
        to = zed * 4 + lax.rem(ex + d, 4)
        return copy(
            rows_ref.at[piece], rows_ref.at[piece], s_p.at[2 + d], r_p.at[piece], col=to
        )

    def piece_arrival(index):
        return copy(mine, rows_ref.at[index], s_p.at[0], r_p.at[index], col=col)

    pack_cols(0)
    send_cols(0)

    @pl.when(row < 2)
    def _():
        @pl.loop(1, COLS)
        def _(d):
            dest = lax.rem(col + d, COLS)
            send_p[dest] = kid_cols[pick_col(dest), 0:B, :]

        recv_p[col] = kid_cols[pick_col(col), 0:B, :]

        @pl.loop(1, COLS)
        def _(d):
            panel_copy(d).start()

    pack_cols(1)
    send_cols(1)
    for g in range(2, PARTS):
        pack_cols(g)

    def direct_copy(g, dy, side):
        chip_to = lax.rem(chip + dy, 4)
        return copy(
            send_r.at[g, chip_to * 3 + side],
            recv_r[g].at[row],
            rs.at[g, dy * 3 + side],
            dr.at[g, row],
            row=chip_to * 2 + side,
        )

    def mate_copy(g):
        return copy(
            send_r.at[g, chip * 3 + other], recv_r[g].at[row], rs.at[g, 0], dr.at[g, row], row=mate
        )

    def extra_copy(g, dy):
        chip_to = lax.rem(chip + dy, 4)
        return copy(
            send_r.at[g, chip_to * 3 + 2],
            recv_r[g].at[8 + row],
            rs.at[g, dy * 3 + 2],
            br.at[g, row],
            row=chip_to * 2 + core,
        )

    def row_arrival(g, source, base, sem):
        return copy(
            send_r.at[g, 0], recv_r[g].at[base + source], rs.at[g, 0], sem.at[g, source], row=source
        )

    def forward_copy(g, dy):
        source = lax.rem(chip + dy, 4) * 2 + core
        return copy(
            recv_r[g].at[8 + source],
            recv_r[g].at[8 + source],
            fs.at[g, dy],
            br.at[g, source],
            row=mate,
        )

    def await_cols(g):
        each_col(g, lambda d, start: col_arrival(g, d, start).wait_recv())

    def spread_rows(g):
        sources = []
        for h in range(2):
            for b in range(6):
                j = jnp.maximum(tab[T_INV + h * 96 + col * 6 + b], 0)
                sources.append(h * 8 + lax.rem(j, 8))

        @pl.loop(0, 12)
        def _(q):
            for h in range(2):
                k = tab[T_ROW + (h * 8 + row) * 12 + q]
                for b in range(6):
                    send_r[g, q, h, :, b * B : (b + 1) * B] = recv_c[g][sources[h * 6 + b], k]

        recv_r[g][row] = send_r[g, chip * 3 + core]
        recv_r[g][8 + row] = send_r[g, chip * 3 + 2]
        for dy in (2, 1, 3):
            extra_copy(g, dy).start()
            direct_copy(g, dy, 0).start()
            direct_copy(g, dy, 1).start()
        mate_copy(g).start()
        forward_copy(g, 0).start()

    def forward(g):
        for dy in range(1, 4):
            row_arrival(g, lax.rem(chip + dy, 4) * 2 + core, 8, br).wait_recv()
            forward_copy(g, dy).start()

    lane = lax.broadcasted_iota(jnp.int32, (1, B), 1)

    def land(g):
        for d in range(1, ROWS):
            row_arrival(g, lax.rem(row + d, ROWS), 0, dr).wait_recv()
        for dy in range(4):
            row_arrival(g, lax.rem(chip + dy, 4) * 2 + other, 8, br).wait_recv()
        alive = []
        for h in range(2):
            for b in range(6):
                j = tab[T_INV + h * 96 + col * 6 + b]
                limit = jnp.where(j < 0, 0, tab[T_ORD + h] - j * B)
                if b < 2:
                    limit = jnp.where(col == 0, 0, limit)
                alive.append(lane < limit)
        down = lax.broadcasted_iota(jnp.int32, (SUB, 1), 0) + g * SUB

        @pl.loop(0, 12)
        def _(a):
            start = pl.multiple_of(a * B + g * SUB, SUB)
            picks, lives = [], []
            for h in range(2):
                place = h * 96 + row * 12 + a
                i = tab[T_INV + place]
                limit = jnp.where(i < 0, 0, tab[T_ORD + h] - i * B)
                limit = jnp.where(row * 12 + a < 2, 0, limit)
                picks.append(tab[T_SEL + place])
                lives.append(down < limit)
            for b in range(6):
                span = slice(b * B, (b + 1) * B)
                total = out[pl.ds(start, SUB), span]
                for h in range(2):
                    part = recv_r[g][picks[h], h, :, span]
                    total = total + jnp.where(lives[h] & alive[h * 6 + b], part, 0.0)
                out[pl.ds(start, SUB), span] = total

    def frame(place, who, b):
        total = jnp.zeros((B, B), jnp.float32)
        for h in range(2):
            j = tab[T_INV + h * 96 + col * 6 + b]
            source = h * 8 + lax.rem(jnp.maximum(j, 0), 8)
            limit = jnp.where(j < 0, 0, tab[T_ORD + h] - j * B)
            limit = jnp.where(tab[T_INV + h * 96 + place] == who, limit, 0)
            total = total + jnp.where(lane < limit, recv_p[source], 0.0)
        return total

    tall = lax.broadcasted_iota(jnp.int32, (B, B), 0)
    wide = lax.broadcasted_iota(jnp.int32, (B, B), 1)

    def gather_panel():
        @pl.when(row < 2)
        def _():
            @pl.loop(1, COLS)
            def _(d):
                panel_arrival(d).wait_recv()

            @pl.loop(0, COLS)
            def _(source):
                for g in range(1, PARTS):
                    recv_c[g][source, 0] = recv_p[source, g * SUB : (g + 1) * SUB, :]

        @pl.when(row == 1)
        def _():
            for b in range(6):
                late[:, b * B : (b + 1) * B] = frame(1, 1, b)
            late_copy().start()

        @pl.when(top)
        def _():
            for place in range(2):
                here = slice(place * B, (place + 1) * B)
                for b in range(6):
                    span = slice(b * B, (b + 1) * B)
                    mine[here, span] = out[here, span] + frame(place, 0, b)
            late_arrival().wait_recv()
            mine[B:, :] = mine[B:, :] + late[...]

        @pl.when(top)
        def _():
            for d in (2, 6, 1):
                mine_copy(d, row=d).start()

        share_corner_x(top)

    def share_mine():
        for d in (2, 1, 3):
            z_copy(d).start()
        rows_ref[piece] = mine[...]

    def share_corner_x(who):
        @pl.when(who & (col == 0))
        def _():
            for d in (2, 1, 3):
                corner_x(d).start()
            corner[...] = mine[:, 0:NPIV]

    def share_corner_z(who):
        @pl.when(who & (col > 0) & (col < 4))
        def _():
            corner_arrival().wait_recv()

        @pl.when(who & (col < 4))
        def _():
            for d in (2, 1, 3):
                corner_z(d).start()

    def share_corner_mate(who):
        @pl.when(who & (col > 3))
        def _():
            corner_arrival().wait_recv()

        @pl.when(who)
        def _():
            corner_mate().start()

    def half_copy(n):
        half = mine.at[n * B : (n + 1) * B]
        return copy(half, half, s_u.at[3], misc.at[3 + n], row=4)

    def take_mine(who):
        @pl.when(who & (row != 4))
        def _():
            mine_copy(0, row=row).wait_recv()

        @pl.when(who & (row == 2))
        def _():
            half_copy(0).start()

        @pl.when(who & (row == 6))
        def _():
            half_copy(1).start()

        @pl.when(who & (row == 4))
        def _():
            half_copy(0).wait_recv()
            half_copy(1).wait_recv()

        share_corner_x(who & (core == 0))

        @pl.when(who & (core == 0))
        def _():
            mine_copy(4, row=row + 1).start()

    def share_z(who):
        @pl.when(who & owner)
        def _():
            share_mine()

    def share_rows(who):
        @pl.when(who & holder & jnp.logical_not(owner))
        def _():
            piece_arrival(piece).wait_recv()

        @pl.when(who & holder)
        def _():
            for d in (2, 1, 3):
                x_copy(d).start()

    below = row > 1

    def panel_step(g):
        if g == 0:
            gather_panel()
        if g == 1:
            take_mine(row == 1)
        if g == 2:
            share_corner_z(top)
            take_mine(relay & (row != 4))
        if g == 3:
            take_mine(row == 4)
            take_mine(below & (core == 1) & (row != 5))
        if g == 4:
            take_mine(row == 5)
            share_corner_mate(top)
            share_corner_z(relay)
        if g == 5:
            share_corner_mate(relay)
        if g == Z_EVEN:
            share_z(core == 0)
        if g == Z_ODD:
            share_z(core == 1)
        if g == X_EVEN:
            share_rows(core == 0)
        if g == X_ODD:
            share_rows(core == 1)

    def first_block():
        @pl.when(core == 1)
        def _():
            corner_arrival().wait_recv()

        work[:, :B] = corner[:B, :B]
        work[:, B:] = (tall == wide).astype(jnp.float32)
        eliminate(work, 0, B - 1)
        up, low_inv = eliminated(work)
        low21 = mul(corner[B:, :B], low_inv, 1, 1)
        inv[:B, :B] = low_inv
        inv[:B, B:] = jnp.zeros((B, B), jnp.float32)
        lower[:B, :B] = up.T
        lower[:B, B:] = jnp.zeros((B, B), jnp.float32)
        lower[B:, :B] = low21
        work[:, :B] = corner[B:, B:] - mul(low21, low21, 1, 1)
        work[:, B:] = (tall == wide).astype(jnp.float32)

    def second_block():
        eliminate(work, 0, B - 1)
        up, low_inv = eliminated(work)
        inv[B:, B:] = low_inv
        inv[B:, :B] = -mul(low_inv, mul(lower[B:, :B], inv[:B, :B], 1, 0), 1, 0)
        lower[B:, B:] = up.T

    def solve_own():
        right[...] = mul(inv[...], mine[...], 1, 0)

    def solve_rows():
        for index in range(2):

            @pl.when(jnp.logical_not(holder & (piece == index)))
            def _():
                piece_arrival(index).wait_recv()

            left[index] = mul(inv[...], rows_ref[index], 1, 0)

    def update():
        @pl.loop(0, 6)
        def _(n):
            block = left[n // 3, :, pl.ds(pl.multiple_of(lax.rem(n, 3) * NPIV, NPIV), NPIV)]
            here = pl.ds(pl.multiple_of(n * NPIV, NPIV), NPIV)
            out[here, :] = out[here, :] - mul(block, right[...], 0, 0)

            @pl.when(col == 0)
            def _():
                out[here, 0:NPIV] = block.T

        @pl.when(top)
        def _():
            out[0:NPIV, :] = jnp.zeros((NPIV, out.shape[1]), jnp.float32)

        @pl.when(first)
        def _():
            out[0:NPIV, 0:NPIV] = lower[...]

    for g in range(PARTS):
        await_cols(g)
        spread_rows(g)
        if g + 2 < PARTS:
            send_cols(g + 2)
        panel_step(g)
        if g >= 3:
            forward(g - 3)
        if g >= 4:
            land(g - 4)
        if g == 5:
            first_block()
        if g == 6:
            second_block()
        if g == 7:
            solve_own()
    panel_step(PARTS)
    for g in range(PARTS - 3, PARTS - 1):
        forward(g)
    for g in range(PARTS - 4, PARTS - 2):
        land(g)
    solve_rows()
    update()
    land(PARTS - 2)
    forward(PARTS - 1)
    land(PARTS - 1)

    for g in range(PARTS):

        each_col(g, lambda d, start: col_copy(g, d, start).wait_send())

        for dy in range(1, 4):
            direct_copy(g, dy, 0).wait_send()
            direct_copy(g, dy, 1).wait_send()
            extra_copy(g, dy).wait_send()
        mate_copy(g).wait_send()
        for dy in range(4):
            forward_copy(g, dy).wait_send()

    @pl.when(row < 2)
    def _():
        @pl.loop(1, COLS)
        def _(d):
            panel_copy(d).wait_send()

    @pl.when(row == 1)
    def _():
        late_copy().wait_send()

    @pl.when((core == 0) & (col == 0))
    def _():
        for d in range(1, 4):
            corner_x(d).wait_send()

    @pl.when((core == 0) & (col < 4))
    def _():
        for d in range(1, 4):
            corner_z(d).wait_send()

    @pl.when(core == 0)
    def _():
        corner_mate().wait_send()

    @pl.when(top)
    def _():
        for d in (2, 6, 1):
            mine_copy(d, row=d).wait_send()

    @pl.when(relay)
    def _():
        mine_copy(4, row=row + 1).wait_send()

    @pl.when(row == 2)
    def _():
        half_copy(0).wait_send()

    @pl.when(row == 6)
    def _():
        half_copy(1).wait_send()

    @pl.when(owner)
    def _():
        for d in (2, 1, 3):
            z_copy(d).wait_send()

    @pl.when(holder)
    def _():
        for d in (2, 1, 3):
            x_copy(d).wait_send()


def shards(parent_front, child_blocks, child_map, child_order):
    table = routing_table(child_map, child_order)
    width = parent_front.shape[1]
    wild = pl.BlockSpec(memory_space=pl.ANY)

    def vmem(*shape):
        return pltpu.VMEM(shape, jnp.float32)

    dma = pltpu.SemaphoreType.DMA
    return pl.pallas_call(
        front_kernel,
        out_shape=pltpu.VMEM(parent_front.shape, jnp.float32),
        in_specs=[pl.BlockSpec(memory_space=pltpu.SMEM), wild, wild],
        out_specs=pl.BlockSpec(memory_space=pltpu.VMEM),
        scratch_shapes=[
            vmem(8, 8 * B, B),
            vmem(PARTS, COLS, 8, SUB, B),
            vmem(PARTS, 12, 2, SUB, width),
            vmem(COLS, B, B),
            vmem(COLS, B, B),
            vmem(B, width),
            vmem(NPIV, NPIV),
            vmem(NPIV, width),
            vmem(2, NPIV, width),
            vmem(B, 2 * B),
            vmem(NPIV, NPIV),
            vmem(NPIV, NPIV),
            vmem(2, NPIV, width),
            vmem(NPIV, width),
            dma((9,)),
            dma((PARTS, COLS)),
            dma((PARTS, COLS)),
            dma((PARTS, 12)),
            dma((PARTS, ROWS)),
            dma((PARTS, ROWS)),
            dma((PARTS, 4)),
            dma((COLS,)),
            dma((COLS,)),
            dma((7,)),
            dma((8,)),
            dma((6,)),
            dma((2,)),
            dma((5,)),
        ]
        + [vmem(COLS, 8, SUB, B)] * PARTS
        + [vmem(16, 2, SUB, width)] * PARTS,
        compiler_params=pltpu.CompilerParams(
            collective_id=0, has_side_effects=True, vmem_limit_bytes=VMEM_LIMIT
        ),
        name="front",
    )(table, parent_front, child_blocks)


def solution(mesh):
    placed = (P("row", "col"), P("row", "col"), P(), P())
    return jax.shard_map(
        shards, mesh=mesh, in_specs=placed, out_specs=P("row", "col"), check_vma=False
    )
```
